16 devices in a mesh: rep: 4 (over y, z, core), dp: 4 (over x).
Axes of the slice: x: 4, y: 2, z: 1, core: 2. Of those that a mesh axis runs over, the one named last changes fastest.
The devices are a block of a 4x4x8 slice.
Arguments:
- x: bfloat16 [16, 4096, 768], P(('rep', 'dp')), parts along dimension 0
- dy: bfloat16 [16, 4096, 768], P(('rep', 'dp')), parts along dimension 0
- w_gate: bfloat16 [2, 768, 1792], P(None, 'dp')
- w_up: bfloat16 [2, 768, 1792], P(None, 'dp')
- w_down: bfloat16 [2, 1792, 768], P(None, 'dp')
Outputs:
- output 1: bfloat16 [16, 4096, 768], P(('rep', 'dp')), parts along dimension 0
- output 2: bfloat16 [8, 768, 1792], P('rep', 'dp'), parts along dimension 0
- output 3: bfloat16 [8, 768, 1792], P('rep', 'dp'), parts along dimension 0
- output 4: bfloat16 [8, 1792, 768], P('rep', 'dp'), parts along dimension 0
There are 4 independent parts. The reference program is written for one: setup_inputs(seed, part) draws one part's arguments, and reference() takes and returns one part's arrays. A program takes and returns all parts, laid end to end along the dimension named above; an argument that names none is the same for every part.
All inputs are finite; a program needn't handle non-finite values.
Results may differ from the reference program's by a relative error of at most 0.018.
Values are sent between devices in bfloat16 or wider.
A program may use at most 768 MiB of HBM per device.

```python
import jax
import jax.numpy as jnp
from jax import lax

SEQUENCES = 4
TOKENS = 4096
D = 768
FF = 1792
LAYERS = 2
NAMES = ("w_gate", "w_up", "w_down")
SHAPES = {"w_gate": (LAYERS, D, FF), "w_up": (LAYERS, D, FF), "w_down": (LAYERS, FF, D)}


def bump(key, n, height):
    away = (jnp.arange(n, dtype=jnp.int32) - jax.random.randint(key, (), 0, n, jnp.int32)) % n
    return jnp.where(away < n // 8, height, 1.0)


def together(key, own, strength):
    shared = jax.random.normal(key, own.shape[1:], jnp.float32)
    return (own + strength * shared) * lax.rsqrt(1 + strength * strength)


def setup_inputs(seed: int = 0, part: int = 0) -> dict:
    kx, kdy, ka, kb, kz, kf, kh, kl, *kw = jax.random.split(jax.random.key(seed), 8 + len(NAMES))
    kx, kdy, ka, kb = (jax.random.fold_in(k, part) for k in (kx, kdy, ka, kb))
    shape = (SEQUENCES, TOKENS, D)
    much_x, much_dy = jax.random.uniform(kz, (2,), jnp.float32, 0.0, 1.0)
    layers = 2.0 ** jax.random.uniform(kl, (LAYERS, 1, 1), jnp.float32, -1.0, 1.0)
    x = together(ka, jax.random.normal(kx, shape, jnp.float32), much_x) * bump(kf, D, 4.0)
    dy = together(kb, jax.random.normal(kdy, shape, jnp.float32), much_dy)
    drawn = {"x": x.astype(jnp.bfloat16), "dy": (dy * (SEQUENCES * TOKENS) ** -0.5).astype(jnp.bfloat16)}
    for key, name in zip(kw, NAMES, strict=True):
        w = jax.random.normal(key, SHAPES[name], jnp.float32) * SHAPES[name][1] ** -0.5
        drawn[name] = (w * {"w_gate": 1.0, "w_up": bump(kh, FF, 4.0), "w_down": layers}[name]).astype(jnp.bfloat16)
    return drawn


def matmul(a, w):
    return jnp.dot(a, w, preferred_element_type=jnp.float32).astype(jnp.bfloat16)


def normed(h):
    wide = h.astype(jnp.float32)
    scale = lax.rsqrt(jnp.mean(wide**2, -1, keepdims=True) + 1e-6)
    return (wide * scale).astype(jnp.bfloat16)


def layer(h, w):
    a = normed(h)
    gate = jnp.dot(a, w["w_gate"], preferred_element_type=jnp.float32)
    up = jnp.dot(a, w["w_up"], preferred_element_type=jnp.float32)
    return h + matmul((jax.nn.silu(gate) * up).astype(jnp.bfloat16), w["w_down"])


def stack(weights, h):
    return lax.scan(lambda h, w: (layer(h, w), None), h, weights)[0]


def reference(x, dy, w_gate, w_up, w_down):
    weights = dict(zip(NAMES, (w_gate, w_up, w_down), strict=True))

    def take(so_far, sequence):
        h, by_y = sequence
        _, back = jax.vjp(stack, weights, h)
        by_weights, by_h = back(by_y)
        return jax.tree.map(lambda total, term: total + term.astype(jnp.float32), so_far, by_weights), by_h

    none_yet = {name: jnp.zeros(w.shape, jnp.float32) for name, w in weights.items()}
    by_weights, by_x = lax.scan(take, none_yet, (x, dy))
    return (by_x, *(by_weights[name].astype(jnp.bfloat16) for name in NAMES))
```

```python
import functools

import jax
import jax.numpy as jnp
from jax import lax
from jax.experimental import pallas as pl
from jax.experimental.pallas import tpu as pltpu
from jax.sharding import PartitionSpec as P

F32, BF16 = jnp.float32, jnp.bfloat16
NT = (((1,), (1,)), ((), ()))
TN = (((0,), (0,)), ((), ()))
VMEM_LIMIT = 60 * 2**20
TILE = 512
COLS = 256
LATER = {
    2: (("neighbours", 3), ("own", 5)),
    3: (("neighbours", 4), ("opposite", 3)),
    5: (("neighbours", 5), ("opposite", 4)),
    7: (("opposite", 5),),
}


def dot(a, b):
    return jnp.dot(a, b, preferred_element_type=F32)


def dot_as(a, b, dims):
    return lax.dot_general(a, b, dims, preferred_element_type=F32)


def normed(h):
    wide = h.astype(F32)
    scale = lax.rsqrt(jnp.mean(wide * wide, -1, keepdims=True) + 1e-6)
    return wide, scale


def cuts(n, size):
    return [slice(at, min(at + size, n)) for at in range(0, n, size)]


def whole(shape):
    return pl.BlockSpec(shape, lambda *_: (0,) * len(shape), pipeline_mode=pl.Buffered(1))


def rows_of(width, tile=TILE):
    return pl.BlockSpec((tile, width), lambda i: (i, 0))


def params(**more):
    return pltpu.CompilerParams(dimension_semantics=("arbitrary",), vmem_limit_bytes=VMEM_LIMIT, **more)


def cost(matmuls, rows, d, ff, moved):
    return pl.CostEstimate(flops=2 * matmuls * rows * d * ff, bytes_accessed=moved, transcendentals=0)


class Gather:
    def __init__(self, n, shards, fulls, send, recv, local):
        self.n, self.shards, self.fulls, self.send, self.recv, self.local = n, shards, fulls, send, recv, local
        self.me = lax.axis_index("dp")
        rep = lax.axis_index("rep")
        self.core = lax.rem(rep, 2)
        self.partner = {"rep": rep + 1 - 2 * self.core}
        self.right = {"dp": lax.rem(self.me + 1, n)}
        self.left = {"dp": lax.rem(self.me + n - 1, n)}

    def shard(self, m):
        ref = self.shards[m % 3]
        return ref.at[m // 3]

    def piece(self, m, away, quarter=None):
        block = self.shards[m % 3].shape[1]
        half = block // 2
        at = lax.rem(self.me + away + self.n, self.n) * block + self.core * half
        if quarter is None:
            return self.fulls[m].at[pl.ds(at, half)]
        return self.fulls[m].at[pl.ds(at + quarter * (half // 2), half // 2)]

    def other_piece(self, m, away, quarter=None):
        block = self.shards[m % 3].shape[1]
        half = block // 2
        at = lax.rem(self.me + away + self.n, self.n) * block + (1 - self.core) * half
        if quarter is None:
            return self.fulls[m].at[pl.ds(at, half)]
        return self.fulls[m].at[pl.ds(at + quarter * (half // 2), half // 2)]

    def copy(self, m, k, src, dst, to):
        return pltpu.make_async_remote_copy(
            src_ref=src, dst_ref=dst, send_sem=self.send.at[m, k], recv_sem=self.recv.at[m, k],
            device_id=to, device_id_type=pl.DeviceIdType.MESH,
        )

    def sends(self, m, k):
        if k < 2:
            block = self.shards[m % 3].shape[1]
            src = self.shard(m).at[pl.ds(self.core * (block // 2), block // 2)]
            return self.copy(m, k, src, self.piece(m, 0), (self.right, self.left)[k])
        part = {2: (-1, 0), 3: (1, 1), 4: (-1, None), 5: (1, None), 6: (2, 0), 7: (2, 1)}[k]
        ref = self.piece(m, *part)
        return self.copy(m, k, ref, ref, (self.right, self.left)[k - 2] if k < 4 else self.partner)

    def arrives(self, m, k):
        if k < 4:
            part = ((-1, None), (1, None), (2, 0), (2, 1))[k]
            ref = self.piece(m, *part)
        else:
            part = {4: (-1, None), 5: (1, None), 6: (2, 0), 7: (2, 1)}[k]
            ref = self.other_piece(m, *part)
        return self.copy(m, k, ref, ref, self.partner)

    def mine(self, m):
        block = self.shards[m % 3].shape[1]
        return pltpu.make_async_copy(self.shard(m), self.fulls[m].at[pl.ds(self.me * block, block)], self.local.at[m])

    def greet(self):
        barrier = pltpu.get_barrier_semaphore()
        for other in (self.left, self.right, self.partner):
            pl.semaphore_signal(barrier, inc=1, device_id=other, device_id_type=pl.DeviceIdType.MESH)
        pl.semaphore_wait(barrier, 3)

    def start(self, m, ks):
        for k in ks:
            self.sends(m, k).start()

    def own(self, m):
        self.start(m, (0, 1))
        self.mine(m).start()

    def neighbours(self, m):
        self.arrives(m, 0).wait_recv()
        self.start(m, (2, 4))
        self.arrives(m, 1).wait_recv()
        self.start(m, (3, 5))

    def opposite(self, m):
        self.arrives(m, 2).wait_recv()
        self.start(m, (6,))
        self.arrives(m, 3).wait_recv()
        self.start(m, (7,))

    def complete(self, m):
        self.mine(m).wait()
        for k in range(4, 8):
            self.arrives(m, k).wait_recv()

    def sent(self, m):
        for k in range(8):
            self.sends(m, k).wait_send()


def forward_kernel(n, x, sg, su, sd, h1, act, g_out, u_out, *rest):
    outs, fulls, (send, recv, local, out_sem) = rest[:6], rest[6:12], rest[12:]
    gather = Gather(n, (sg, su, sd), fulls, send, recv, local)
    step = pl.program_id(0)

    def keep(m):
        return pltpu.make_async_copy(fulls[m], outs[m], out_sem.at[m])

    @pl.when(step == 0)
    def _():
        gather.greet()
        gather.own(0)
        gather.own(1)
        gather.neighbours(0)
        gather.own(2)
        gather.neighbours(1)
        gather.opposite(0)
        gather.own(3)
        gather.neighbours(2)
        gather.opposite(1)
        gather.own(4)
        gather.opposite(2)
        for m in range(3):
            gather.complete(m)
            keep(m).start()

    for at, events in LATER.items():
        @pl.when(step == at)
        def _():
            for stage, m in events:
                getattr(gather, stage)(m)

    wg, wu, wd = fulls[:3]
    h = x[...]
    wide, scale = normed(h)
    a = (wide * scale).astype(BF16)
    for s in cuts(wg.shape[1], COLS):
        g = dot(a, wg[:, s])
        u = dot(a, wu[:, s])
        g_out[:, s] = g
        u_out[:, s] = u
        act[:, s] = (g * jax.nn.sigmoid(g) * u).astype(BF16)
    h1[...] = h + dot(act[...], wd[...]).astype(BF16)

    @pl.when(step == pl.num_programs(0) - 1)
    def _():
        for m in range(3, 6):
            gather.complete(m)
            keep(m).start()
        for m in range(6):
            gather.sent(m)
            keep(m).wait()


def forward(n, x, sg, su, sd):
    rows, d = x.shape
    ff = sg.shape[2]
    shapes = [(d, ff), (d, ff), (ff, d)] * 2
    outs = [((rows, d), BF16), ((rows, ff), BF16), ((rows, ff), F32), ((rows, ff), F32)] + [(s, BF16) for s in shapes]
    anywhere = pl.BlockSpec(memory_space=pl.ANY)
    assert rows // TILE == 8 and n == 4
    return pl.pallas_call(
        functools.partial(forward_kernel, n),
        grid=(rows // TILE,),
        out_shape=[jax.ShapeDtypeStruct(*o) for o in outs],
        in_specs=[rows_of(d)] + [anywhere] * 3,
        out_specs=[rows_of(d), rows_of(ff), rows_of(ff), rows_of(ff)] + [anywhere] * 6,
        scratch_shapes=[pltpu.VMEM(s, BF16) for s in shapes]
        + [pltpu.SemaphoreType.DMA((6, 8)), pltpu.SemaphoreType.DMA((6, 8)), pltpu.SemaphoreType.DMA((6,)), pltpu.SemaphoreType.DMA((6,))],
        compiler_params=params(collective_id=0, has_side_effects=True),
        cost_estimate=cost(3, rows, d, ff, 100 * 2**20),
        name="forward",
    )(x, sg, su, sd)


def through_norm(wide, scale, da, dh):
    m = jnp.mean(da * wide, -1, keepdims=True)
    return dh + (scale * da - wide * (scale * scale * scale * m)).astype(BF16)


def gate_grads(g, u, dact):
    sig = jax.nn.sigmoid(g)
    silu = g * sig
    return silu, (dact * u * (sig + silu * (1 - sig))).astype(BF16), (dact * silu).astype(BF16)


def last_kernel(h_ref, dy_ref, wg, wu, wd, dh, act, dg, du):
    wide, scale = normed(h_ref[...])
    a = (wide * scale).astype(BF16)
    dy = dy_ref[...]
    for s in cuts(wg.shape[1], COLS):
        g = dot(a, wg[:, s])
        u = dot(a, wu[:, s])
        dact = dot_as(dy, wd[s, :], NT).astype(BF16).astype(F32)
        silu, dg[:, s], du[:, s] = gate_grads(g, u, dact)
        act[:, s] = (silu * u).astype(BF16)
    da = dot_as(dg[...], wg[...], NT) + dot_as(du[...], wu[...], NT)
    dh[...] = through_norm(wide, scale, da.astype(BF16).astype(F32), dy)


def last(h, dy, wg, wu, wd):
    rows, d = h.shape
    ff = wg.shape[1]
    return pl.pallas_call(
        last_kernel,
        grid=(rows // TILE,),
        out_shape=[jax.ShapeDtypeStruct((rows, d), BF16)] + [jax.ShapeDtypeStruct((rows, ff), BF16)] * 3,
        in_specs=[rows_of(d), rows_of(d)] + [whole(w.shape) for w in (wg, wu, wd)],
        out_specs=[rows_of(d)] + [rows_of(ff)] * 3,
        compiler_params=params(),
        cost_estimate=cost(5, rows, d, ff, 80 * 2**20),
        name="last",
    )(h, dy, wg, wu, wd)


def first_kernel(h_ref, dh1_ref, g_ref, u_ref, wg, wu, wd, dx, dg, du):
    wide, scale = normed(h_ref[...])
    dh1 = dh1_ref[...]
    for s in cuts(wg.shape[1], COLS):
        dact = dot_as(dh1, wd[s, :], NT).astype(BF16).astype(F32)
        _, dg[:, s], du[:, s] = gate_grads(g_ref[:, s], u_ref[:, s], dact)
    da = dot_as(dg[...], wg[...], NT) + dot_as(du[...], wu[...], NT)
    dx[...] = through_norm(wide, scale, da.astype(BF16).astype(F32), dh1)


def first(h, dh1, g, u, wg, wu, wd):
    rows, d = h.shape
    ff = wg.shape[1]
    return pl.pallas_call(
        first_kernel,
        grid=(rows // TILE,),
        out_shape=[jax.ShapeDtypeStruct((rows, d), BF16)] + [jax.ShapeDtypeStruct((rows, ff), BF16)] * 2,
        in_specs=[rows_of(d), rows_of(d), rows_of(ff), rows_of(ff)] + [whole(w.shape) for w in (wg, wu, wd)],
        out_specs=[rows_of(d)] + [rows_of(ff)] * 2,
        compiler_params=params(),
        cost_estimate=cost(3, rows, d, ff, 110 * 2**20),
        name="first",
    )(h, dh1, g, u, wg, wu, wd)


def in_kernel(h_ref, grad_ref, out, total):
    step = pl.program_id(0)

    @pl.when(step == 0)
    def _():
        total[...] = jnp.zeros_like(total)

    wide, scale = normed(h_ref[...])
    a = (wide * scale).astype(BF16)
    for s in cuts(grad_ref.shape[1], COLS):
        total[:, s] += dot_as(a, grad_ref[:, s], TN)

    @pl.when(step == pl.num_programs(0) - 1)
    def _():
        out[...] = total[...].astype(BF16)


def grad_in(h, grad, name, tile=1024):
    rows, d = h.shape
    ff = grad.shape[1]
    return pl.pallas_call(
        in_kernel,
        grid=(rows // tile,),
        out_shape=jax.ShapeDtypeStruct((d, ff), BF16),
        in_specs=[rows_of(d, tile), rows_of(ff, tile)],
        out_specs=whole((d, ff)),
        scratch_shapes=[pltpu.VMEM((d, ff), F32)],
        compiler_params=params(),
        cost_estimate=cost(1, rows, d, ff, 24 * 2**20),
        name=name,
    )(h, grad)


def out_kernel(act_ref, dh_ref, out):
    out[...] = dot_as(act_ref[...], dh_ref[...], TN).astype(BF16)


def grad_out(act, dh, name):
    rows, ff = act.shape
    d = dh.shape[1]
    return pl.pallas_call(
        out_kernel,
        grid=(ff // COLS,),
        out_shape=jax.ShapeDtypeStruct((ff, d), BF16),
        in_specs=[pl.BlockSpec((rows, COLS), lambda i: (0, i)), whole((rows, d))],
        out_specs=pl.BlockSpec((COLS, d), lambda i: (i, 0)),
        compiler_params=params(),
        cost_estimate=cost(1, rows, d, ff, 24 * 2**20),
        name=name,
    )(act, dh)


def solution(mesh):
    n = mesh.shape["dp"]

    def scatter(term):
        return lax.psum_scatter(term, "dp", scatter_dimension=0, tiled=True)

    def body(x, dy, sg, su, sd):
        x, dy = x[0], dy[0]
        h1, act0, g0, u0, wg0, wu0, wd0, wg1, wu1, wd1 = forward(n, x, sg, su, sd)
        dh1, act1, dg1, du1 = last(h1, dy, wg1, wu1, wd1)
        down1 = scatter(grad_out(act1, dy, "down1"))
        gate1 = scatter(grad_in(h1, dg1, "gate1"))
        up1 = scatter(grad_in(h1, du1, "up1"))
        down0 = scatter(grad_out(act0, dh1, "down0"))
        dx, dg0, du0 = first(x, dh1, g0, u0, wg0, wu0, wd0)
        gate0 = scatter(grad_in(x, dg0, "gate0"))
        up0 = scatter(grad_in(x, du0, "up0"))
        return dx[None], jnp.stack([gate0, gate1]), jnp.stack([up0, up1]), jnp.stack([down0, down1])

    tokens = P(("rep", "dp"), None, None)
    return jax.shard_map(
        body,
        mesh=mesh,
        in_specs=(tokens, tokens) + (P(None, "dp", None),) * 3,
        out_specs=(tokens,) + (P("rep", "dp", None),) * 3,
        check_vma=False,
    )
```

```python
import functools

import jax
import jax.numpy as jnp
from jax import lax
from jax.experimental import pallas as pl
from jax.experimental.pallas import tpu as pltpu
from jax.sharding import PartitionSpec as P

F32, BF16 = jnp.float32, jnp.bfloat16
NT = (((1,), (1,)), ((), ()))
TN = (((0,), (0,)), ((), ()))
VMEM_LIMIT = 60 * 2**20
TILE = 512
COLS = 256
SMALL = 256
SLOTS = 6
LATER = {
    2: (("neighbours", 3), ("own", 5)),
    3: (("neighbours", 4), ("opposite", 3)),
    5: (("neighbours", 5), ("opposite", 4)),
    7: (("opposite", 5),),
}


def dot(a, b):
    return jnp.dot(a, b, preferred_element_type=F32)


def dot_as(a, b, dims):
    return lax.dot_general(a, b, dims, preferred_element_type=F32)


def normed(h):
    wide = h.astype(F32)
    scale = lax.rsqrt(jnp.mean(wide * wide, -1, keepdims=True) + 1e-6)
    return wide, scale


def cuts(n, size):
    return [slice(at, min(at + size, n)) for at in range(0, n, size)]


def whole(shape):
    return pl.BlockSpec(shape, lambda *_: (0,) * len(shape), pipeline_mode=pl.Buffered(1))


def rows_of(width, tile=TILE):
    return pl.BlockSpec((tile, width), lambda i: (i, 0))


def params(**more):
    return pltpu.CompilerParams(dimension_semantics=("arbitrary",), vmem_limit_bytes=VMEM_LIMIT, **more)


def cost(matmuls, rows, d, ff, moved):
    return pl.CostEstimate(flops=2 * matmuls * rows * d * ff, bytes_accessed=moved, transcendentals=0)


class Gather:
    def __init__(self, n, shards, fulls, send, recv, local):
        self.n, self.shards, self.fulls, self.send, self.recv, self.local = n, shards, fulls, send, recv, local
        self.me = lax.axis_index("dp")
        rep = lax.axis_index("rep")
        self.core = lax.rem(rep, 2)
        self.partner = {"rep": rep + 1 - 2 * self.core}
        self.right = {"dp": lax.rem(self.me + 1, n)}
        self.left = {"dp": lax.rem(self.me + n - 1, n)}

    def shard(self, m):
        ref = self.shards[m % 3]
        return ref.at[m // 3]

    def piece(self, m, away, quarter=None):
        block = self.shards[m % 3].shape[1]
        half = block // 2
        at = lax.rem(self.me + away + self.n, self.n) * block + self.core * half
        if quarter is None:
            return self.fulls[m].at[pl.ds(at, half)]
        return self.fulls[m].at[pl.ds(at + quarter * (half // 2), half // 2)]

    def other_piece(self, m, away, quarter=None):
        block = self.shards[m % 3].shape[1]
        half = block // 2
        at = lax.rem(self.me + away + self.n, self.n) * block + (1 - self.core) * half
        if quarter is None:
            return self.fulls[m].at[pl.ds(at, half)]
        return self.fulls[m].at[pl.ds(at + quarter * (half // 2), half // 2)]

    def copy(self, m, k, src, dst, to):
        return pltpu.make_async_remote_copy(
            src_ref=src, dst_ref=dst, send_sem=self.send.at[m, k], recv_sem=self.recv.at[m, k],
            device_id=to, device_id_type=pl.DeviceIdType.MESH,
        )

    def sends(self, m, k):
        if k < 2:
            block = self.shards[m % 3].shape[1]
            src = self.shard(m).at[pl.ds(self.core * (block // 2), block // 2)]
            return self.copy(m, k, src, self.piece(m, 0), (self.right, self.left)[k])
        part = {2: (-1, 0), 3: (1, 1), 4: (-1, None), 5: (1, None), 6: (2, 0), 7: (2, 1)}[k]
        ref = self.piece(m, *part)
        return self.copy(m, k, ref, ref, (self.right, self.left)[k - 2] if k < 4 else self.partner)

    def arrives(self, m, k):
        if k < 4:
            part = ((-1, None), (1, None), (2, 0), (2, 1))[k]
            ref = self.piece(m, *part)
        else:
            part = {4: (-1, None), 5: (1, None), 6: (2, 0), 7: (2, 1)}[k]
            ref = self.other_piece(m, *part)
        return self.copy(m, k, ref, ref, self.partner)

    def mine(self, m):
        block = self.shards[m % 3].shape[1]
        return pltpu.make_async_copy(self.shard(m), self.fulls[m].at[pl.ds(self.me * block, block)], self.local.at[m])

    def greet(self):
        barrier = pltpu.get_barrier_semaphore()
        for other in (self.left, self.right, self.partner):
            pl.semaphore_signal(barrier, inc=1, device_id=other, device_id_type=pl.DeviceIdType.MESH)
        pl.semaphore_wait(barrier, 3)

    def start(self, m, ks):
        for k in ks:
            self.sends(m, k).start()

    def own(self, m):
        self.start(m, (0, 1))
        self.mine(m).start()

    def neighbours(self, m):
        self.arrives(m, 0).wait_recv()
        self.start(m, (2, 4))
        self.arrives(m, 1).wait_recv()
        self.start(m, (3, 5))

    def opposite(self, m):
        self.arrives(m, 2).wait_recv()
        self.start(m, (6,))
        self.arrives(m, 3).wait_recv()
        self.start(m, (7,))

    def complete(self, m):
        self.mine(m).wait()
        for k in range(4, 8):
            self.arrives(m, k).wait_recv()

    def sent(self, m):
        for k in range(8):
            self.sends(m, k).wait_send()


def forward_kernel(n, x, sg, su, sd, h1, a_out, act, g_out, u_out, *rest):
    outs, fulls, (send, recv, local, out_sem) = rest[:6], rest[6:12], rest[12:]
    gather = Gather(n, (sg, su, sd), fulls, send, recv, local)
    step = pl.program_id(0)

    def keep(m):
        return pltpu.make_async_copy(fulls[m], outs[m], out_sem.at[m])

    @pl.when(step == 0)
    def _():
        gather.greet()
        gather.own(0)
        gather.own(1)
        gather.neighbours(0)
        gather.own(2)
        gather.neighbours(1)
        gather.opposite(0)
        gather.own(3)
        gather.neighbours(2)
        gather.opposite(1)
        gather.own(4)
        gather.opposite(2)
        for m in range(3):
            gather.complete(m)
            keep(m).start()

    for at, events in LATER.items():
        @pl.when(step == at)
        def _():
            for stage, m in events:
                getattr(gather, stage)(m)

    wg, wu, wd = fulls[:3]
    h = x[...]
    wide, scale = normed(h)
    a = (wide * scale).astype(BF16)
    a_out[...] = a
    for s in cuts(wg.shape[1], COLS):
        g = dot(a, wg[:, s])
        u = dot(a, wu[:, s])
        g_out[:, s] = g
        u_out[:, s] = u
        act[:, s] = (g * jax.nn.sigmoid(g) * u).astype(BF16)
    h1[...] = h + dot(act[...], wd[...]).astype(BF16)

    @pl.when(step == pl.num_programs(0) - 1)
    def _():
        for m in range(3, 6):
            gather.complete(m)
            keep(m).start()
        for m in range(6):
            gather.sent(m)
            keep(m).wait()


def forward(n, x, sg, su, sd):
    rows, d = x.shape
    ff = sg.shape[2]
    shapes = [(d, ff), (d, ff), (ff, d)] * 2
    outs = [((rows, d), BF16), ((rows, d), BF16), ((rows, ff), BF16), ((rows, ff), F32), ((rows, ff), F32)] + [(s, BF16) for s in shapes]
    anywhere = pl.BlockSpec(memory_space=pl.ANY)
    assert rows // TILE == 8 and n == 4
    return pl.pallas_call(
        functools.partial(forward_kernel, n),
        grid=(rows // TILE,),
        out_shape=[jax.ShapeDtypeStruct(*o) for o in outs],
        in_specs=[rows_of(d)] + [anywhere] * 3,
        out_specs=[rows_of(d), rows_of(d), rows_of(ff), rows_of(ff), rows_of(ff)] + [anywhere] * 6,
        scratch_shapes=[pltpu.VMEM(s, BF16) for s in shapes]
        + [pltpu.SemaphoreType.DMA((6, 8)), pltpu.SemaphoreType.DMA((6, 8)), pltpu.SemaphoreType.DMA((6,)), pltpu.SemaphoreType.DMA((6,))],
        compiler_params=params(collective_id=0, has_side_effects=True),
        cost_estimate=cost(3, rows, d, ff, 100 * 2**20),
        name="forward",
    )(x, sg, su, sd)


def through_norm(wide, scale, da, dh):
    m = jnp.mean(da * wide, -1, keepdims=True)
    return dh + (scale * da - wide * (scale * scale * scale * m)).astype(BF16)


def gate_grads(g, u, dact):
    sig = jax.nn.sigmoid(g)
    silu = g * sig
    return silu, (dact * u * (sig + silu * (1 - sig))).astype(BF16), (dact * silu).astype(BF16)


def last_kernel(h_ref, dy_ref, wg, wu, wd, dh, a_out, act, dg, du):
    wide, scale = normed(h_ref[...])
    a = (wide * scale).astype(BF16)
    a_out[...] = a
    dy = dy_ref[...]
    for s in cuts(wg.shape[1], COLS):
        g = dot(a, wg[:, s])
        u = dot(a, wu[:, s])
        dact = dot_as(dy, wd[s, :], NT).astype(BF16).astype(F32)
        silu, dg[:, s], du[:, s] = gate_grads(g, u, dact)
        act[:, s] = (silu * u).astype(BF16)
    da = dot_as(dg[...], wg[...], NT) + dot_as(du[...], wu[...], NT)
    dh[...] = through_norm(wide, scale, da.astype(BF16).astype(F32), dy)


def last(h, dy, wg, wu, wd):
    rows, d = h.shape
    ff = wg.shape[1]
    return pl.pallas_call(
        last_kernel,
        grid=(rows // TILE,),
        out_shape=[jax.ShapeDtypeStruct((rows, d), BF16)] * 2 + [jax.ShapeDtypeStruct((rows, ff), BF16)] * 3,
        in_specs=[rows_of(d), rows_of(d)] + [whole(w.shape) for w in (wg, wu, wd)],
        out_specs=[rows_of(d)] * 2 + [rows_of(ff)] * 3,
        compiler_params=params(),
        cost_estimate=cost(5, rows, d, ff, 80 * 2**20),
        name="last",
    )(h, dy, wg, wu, wd)


class Scatter:
    def __init__(self, n, rows, keep, s1, r1, s2, r2, send, recv):
        self.rows, self.keep, self.s1, self.r1, self.s2, self.r2, self.send, self.recv = rows, keep, s1, r1, s2, r2, send, recv
        self.n = n
        self.me = lax.axis_index("dp")
        self.right = {"dp": lax.rem(self.me + 1, n)}
        self.left = {"dp": lax.rem(self.me + n - 1, n)}

    def copy(self, slot, k, src, dst):
        return pltpu.make_async_remote_copy(
            src_ref=src, dst_ref=dst, send_sem=self.send.at[slot, k], recv_sem=self.recv.at[slot, k],
            device_id=self.left if k % 2 else self.right, device_id_type=pl.DeviceIdType.MESH,
        )

    def opposites(self, slot, k):
        half = self.rows // 2
        return self.copy(slot, k, self.s1.at[slot, pl.ds(k * half, half)], self.r1.at[slot, k])

    def sums(self, slot, k):
        return self.copy(slot, 2 + k, self.s2.at[slot, k], self.r2.at[slot, k])

    def of(self, term, away):
        at = pl.multiple_of(lax.rem(self.me + away, self.n) * self.rows, 64)
        return term[pl.ds(at, self.rows), :]

    def put(self, slot, term):
        self.s1[slot] = self.of(term, 2).astype(BF16)
        self.keep[slot, 0] = self.of(term, 1)
        self.keep[slot, 1] = self.of(term, self.n - 1)
        self.keep[slot, 2] = self.of(term, 0)

    def begin(self, slot):
        for k in range(2):
            self.opposites(slot, k).start()

    def middle(self, slot):
        half = self.rows // 2
        for k in range(2):
            self.opposites(slot, k).wait_recv()
        for k in range(2):
            with_theirs, alone = pl.ds(k * half, half), pl.ds((1 - k) * half, half)
            self.s2[slot, k, with_theirs] = (self.keep[slot, k, with_theirs] + self.r1[slot, k].astype(F32)).astype(BF16)
            self.s2[slot, k, alone] = self.keep[slot, k, alone].astype(BF16)
        for k in range(2):
            self.sums(slot, k).start()

    def end(self, slot):
        for k in range(2):
            self.sums(slot, k).wait_recv()
        out = self.keep[slot, 2] + self.r2[slot, 0].astype(F32) + self.r2[slot, 1].astype(F32)
        for k in range(2):
            self.opposites(slot, k).wait_send()
            self.sums(slot, k).wait_send()
        return out.astype(BF16)


def backward_kernel(
    n, dims, dy, dh1, x, a0, a1, act0, act1, dg1, du1, g0, u0, wg0, wu0, wd0,
    wide_out, down_out, dx, dg0, du0,
    ra, ract, blk, term, wd, g_t, u_t, dh_t, dg_t, du_t, x_t, dx_t,
    wk, ws1, wr1, ws2, wr2, dk, ds1, dr1, ds2, dr2,
    wsend, wrecv, dsend, drecv, blk_sem, res_sem, in_sem, out_sem,
):
    rows, d, ff = dims
    tiles = rows // SMALL
    wides, downs = ff // COLS, d // COLS
    first_tiles = tiles // 2 - downs
    wide = Scatter(n, d // n, wk, ws1, wr1, ws2, wr2, wsend, wrecv)
    down = Scatter(n, ff // n, dk, ds1, dr1, ds2, dr2, dsend, drecv)

    def resident(src, dst, k):
        return pltpu.make_async_copy(src, dst, res_sem.at[k])

    load_a1 = lambda: resident(a1, ra, 0)
    load_a0 = lambda: resident(a0, ra, 0)
    load_act1 = lambda: resident(act1, ract, 1)
    load_act0 = lambda: resident(act0, ract, 1)
    load_wd = lambda: resident(wd0, wd, 2)
    load_wg = lambda: resident(wg0, ract.at[pl.ds(0, d)], 1)
    load_wu = lambda: resident(wu0, ract.at[pl.ds(d, d)], 2)

    def column(src, j, slot):
        return pltpu.make_async_copy(src.at[:, pl.ds(pl.multiple_of(j * COLS, COLS), COLS)], blk.at[slot], blk_sem.at[slot])

    def load_wide(r, i, slot):
        for at, src in ((0, dg1), (1, du1)):
            @pl.when(r == at)
            def _():
                column(src, i, slot).start()

    def load_down(r, j, slot):
        for at, src in ((0, dy), (1, dh1)):
            @pl.when(r == at)
            def _():
                column(src, j, slot).start()

    def load_last(i, slot):
        @pl.when(i < wides)
        def _():
            column(dg0, i, slot).start()

        @pl.when(i >= wides)
        def _():
            column(du0, i - wides, slot).start()

    def tile_of(ref, t):
        return ref.at[pl.ds(pl.multiple_of(t * SMALL, SMALL), SMALL)]

    def tile_in(t):
        slot = lax.rem(t, 2)
        return [pltpu.make_async_copy(tile_of(src, t), dst.at[slot], in_sem.at[k, slot]) for k, (src, dst) in enumerate(((g0, g_t), (u0, u_t), (dh1, dh_t)))]

    def tile_out(t):
        slot = lax.rem(t, 2)
        return [pltpu.make_async_copy(src.at[slot], tile_of(dst, t), out_sem.at[k, slot]) for k, (src, dst) in enumerate(((dg_t, dg0), (du_t, du0)))]

    def tile(t):
        slot = lax.rem(t, 2)
        for c in tile_in(t):
            c.wait()

        @pl.when(t + 1 < tiles)
        def _():
            for c in tile_in(t + 1):
                c.start()

        @pl.when(t >= 2)
        def _():
            for c in tile_out(t - 2):
                c.wait()

        dh = dh_t[slot]
        for s in cuts(ff, COLS):
            dact = dot_as(dh, wd[s, :], NT).astype(BF16).astype(F32)
            _, dg_t[slot, :, s], du_t[slot, :, s] = gate_grads(g_t[slot, :, s], u_t[slot, :, s], dact)
        for c in tile_out(t):
            c.start()

    def late_in(t):
        slot = lax.rem(t, 2)
        pairs = ((dg0, dg_t), (du0, du_t), (dh1, dh_t), (x, x_t))
        return [pltpu.make_async_copy(tile_of(src, t), dst.at[slot], in_sem.at[k, slot]) for k, (src, dst) in enumerate(pairs)]

    def late_out(t):
        slot = lax.rem(t, 2)
        return pltpu.make_async_copy(dx_t.at[slot], tile_of(dx, t), out_sem.at[0, slot])

    def late(t):
        slot = lax.rem(t, 2)
        for c in late_in(t):
            c.wait()

        @pl.when(t + 1 < tiles)
        def _():
            for c in late_in(t + 1):
                c.start()

        @pl.when(t >= 2)
        def _():
            late_out(t - 2).wait()

        h, scale = normed(x_t[slot])
        da = dot_as(dg_t[slot], ract[0:d, :], NT) + dot_as(du_t[slot], ract[d : 2 * d, :], NT)
        dx_t[slot] = through_norm(h, scale, da.astype(BF16).astype(F32), dh_t[slot])
        late_out(t).start()

    def end_wide(k):
        wide_out[k // wides, :, pl.ds(pl.multiple_of(lax.rem(k, wides) * COLS, COLS), COLS)] = wide.end(lax.rem(k, SLOTS))

    def end_down(r, j):
        down_out[r, :, pl.ds(pl.multiple_of(j * COLS, COLS), COLS)] = down.end(j)

    def due_wide(r, i):
        k = wides * r + i

        @pl.when(i >= 2)
        def _():
            wide.middle(lax.rem(k + SLOTS - 2, SLOTS))

        @pl.when((r >= 1) & (i < 2))
        def _():
            down.middle(i + downs - 2)

        @pl.when(i >= 4)
        def _():
            end_wide(k - 4)

        @pl.when((r >= 1) & (i == 0))
        def _():
            end_wide(k - 1)

        @pl.when((r >= 1) & (i >= 1) & (i < 4))
        def _():
            end_down(r - 1, i - 1)

    def due_down(r, j):
        k = wides * r + wides + j

        @pl.when(j < 2)
        def _():
            wide.middle(lax.rem(k - 2, SLOTS))

        @pl.when(j == 2)
        def _():
            down.middle(0)

        end_wide(k - 4)

    def wide_step(r, i, slot, tail):
        term[0:d, :] = dot_as(ra[...], blk[slot], TN)
        k = lax.rem(wides * r + i, SLOTS)
        wide.put(k, term)
        due_wide(r, i)
        tail()
        wide.begin(k)

    load_a1().start()
    load_wide(0, 0, 0)
    load_wd().start()
    for c in tile_in(0):
        c.start()
    load_act1().start()
    barrier = pltpu.get_barrier_semaphore()
    for other in (wide.left, wide.right):
        pl.semaphore_signal(barrier, inc=1, device_id=other, device_id_type=pl.DeviceIdType.MESH)
    pl.semaphore_wait(barrier, 2)
    load_a1().wait()
    load_wd().wait()

    def round_(r, _):
        def wide_block(i, _):
            q = (wides + downs) * r + i
            slot = lax.rem(q, 2)
            column(dg1, 0, slot).wait()

            @pl.when(i + 1 < wides)
            def _():
                load_wide(r, i + 1, 1 - slot)

            @pl.when(i + 1 == wides)
            def _():
                load_down(r, 0, 1 - slot)

            def tail():
                at = (i * first_tiles) // wides

                @pl.when(((i + 1) * first_tiles) // wides > at)
                def _():
                    tile(r * (tiles // 2) + at)

            wide_step(r, i, slot, tail)
            return 0

        lax.fori_loop(0, wides, wide_block, 0)

        @pl.when(r == 1)
        def _():
            load_a0().start()

        load_act1().wait()

        def down_block(j, _):
            q = (wides + downs) * r + wides + j
            slot = lax.rem(q, 2)
            column(dy, 0, slot).wait()

            @pl.when(j + 1 < downs)
            def _():
                load_down(r, j + 1, 1 - slot)

            @pl.when((j + 1 == downs) & (r == 0))
            def _():
                load_wide(r + 1, 0, 1 - slot)

            for s in cuts(ff, ff // 2):
                term[s, :] = dot_as(ract[:, s], blk[slot], TN)
            down.put(j, term)
            due_down(r, j)
            tile(r * (tiles // 2) + first_tiles + j)
            down.begin(j)
            return 0

        lax.fori_loop(0, downs, down_block, 0)

        @pl.when(r == 0)
        def _():
            load_act0().start()

        return 0

    lax.fori_loop(0, 2, round_, 0)

    for t in (tiles - 2, tiles - 1):
        for c in tile_out(t):
            c.wait()
    last_q = 2 * (wides + downs)
    load_last(0, last_q % 2)
    load_wg().start()
    load_wu().start()
    for c in late_in(0):
        c.start()
    load_a0().wait()
    load_wg().wait()
    load_wu().wait()
    blocks = 2 * wides
    late_early = tiles // 2

    def last_block(i, _):
        slot = lax.rem(last_q + i, 2)
        column(dg0, 0, slot).wait()

        @pl.when(i + 1 < blocks)
        def _():
            load_last(i + 1, 1 - slot)

        def tail():
            at = (i * late_early) // blocks

            @pl.when(((i + 1) * late_early) // blocks > at)
            def _():
                late(at)

        wide_step(2, i, slot, tail)
        return 0

    lax.fori_loop(0, blocks, last_block, 0)

    def rest(v, _):
        k = 2 * wides + blocks + v

        def pair(p, _):
            late(late_early + 2 * v + p)
            return 0

        lax.fori_loop(0, 2, pair, 0)

        @pl.when(v < 2)
        def _():
            wide.middle(lax.rem(k - 2, SLOTS))

        end_wide(k - 4)
        return 0

    lax.fori_loop(0, 4, rest, 0)
    for t in (tiles - 2, tiles - 1):
        late_out(t).wait()


def backward(n, dy, dh1, x, a0, a1, act0, act1, dg1, du1, g0, u0, wg0, wu0, wd0):
    rows, d = dy.shape
    ff = act1.shape[1]
    wide, down = d // n, ff // n
    assert n == 4 and rows // SMALL == 16 and d == 3 * COLS and ff == 7 * COLS
    anywhere = pl.BlockSpec(memory_space=pl.ANY)
    inside = pl.BlockSpec(memory_space=pltpu.VMEM)

    def slots(count, chunk):
        return [
            pltpu.VMEM((count, 3, chunk, COLS), F32),
            pltpu.VMEM((count, chunk, COLS), BF16),
            pltpu.VMEM((count, 2, chunk // 2, COLS), BF16),
            pltpu.VMEM((count, 2, chunk, COLS), BF16),
            pltpu.VMEM((count, 2, chunk, COLS), BF16),
        ]

    dma = pltpu.SemaphoreType.DMA
    return pl.pallas_call(
        functools.partial(backward_kernel, n, (rows, d, ff)),
        out_shape=[
            jax.ShapeDtypeStruct((4, wide, ff), BF16),
            jax.ShapeDtypeStruct((2, down, d), BF16),
            jax.ShapeDtypeStruct((rows, d), BF16),
            jax.ShapeDtypeStruct((rows, ff), BF16),
            jax.ShapeDtypeStruct((rows, ff), BF16),
        ],
        in_specs=[anywhere] * 14,
        out_specs=[inside, inside, anywhere, anywhere, anywhere],
        scratch_shapes=[
            pltpu.VMEM((rows, d), BF16),
            pltpu.VMEM((rows, ff), BF16),
            pltpu.VMEM((2, rows, COLS), BF16),
            pltpu.VMEM((ff, COLS), F32),
            pltpu.VMEM((ff, d), BF16),
            pltpu.VMEM((2, SMALL, ff), F32),
            pltpu.VMEM((2, SMALL, ff), F32),
            pltpu.VMEM((2, SMALL, d), BF16),
            pltpu.VMEM((2, SMALL, ff), BF16),
            pltpu.VMEM((2, SMALL, ff), BF16),
            pltpu.VMEM((2, SMALL, d), BF16),
            pltpu.VMEM((2, SMALL, d), BF16),
            *slots(SLOTS, wide),
            *slots(3, down),
            dma((SLOTS, 4)), dma((SLOTS, 4)), dma((3, 4)), dma((3, 4)),
            dma((2,)), dma((3,)), dma((4, 2)), dma((2, 2)),
        ],
        compiler_params=pltpu.CompilerParams(vmem_limit_bytes=67043328, collective_id=1, has_side_effects=True),
        cost_estimate=cost(9, rows, d, ff, 300 * 2**20),
        name="backward",
    )(dy, dh1, x, a0, a1, act0, act1, dg1, du1, g0, u0, wg0, wu0, wd0)


def solution(mesh):
    n = mesh.shape["dp"]

    def body(x, dy, sg, su, sd):
        x, dy = x[0], dy[0]
        h1, a0, act0, g0, u0, wg0, wu0, wd0, wg1, wu1, wd1 = forward(n, x, sg, su, sd)
        dh1, a1, act1, dg1, du1 = last(h1, dy, wg1, wu1, wd1)
        wide, down, dx, _, _ = backward(n, dy, dh1, x, a0, a1, act0, act1, dg1, du1, g0, u0, wg0, wu0, wd0)
        gate1, up1, gate0, up0 = wide
        down1, down0 = down
        return dx[None], jnp.stack([gate0, gate1]), jnp.stack([up0, up1]), jnp.stack([down0, down1])

    tokens = P(("rep", "dp"), None, None)
    return jax.shard_map(
        body,
        mesh=mesh,
        in_specs=(tokens, tokens) + (P(None, "dp", None),) * 3,
        out_specs=(tokens,) + (P("rep", "dp", None),) * 3,
        check_vma=False,
    )
```

```python
import functools

import jax
import jax.numpy as jnp
from jax import lax
from jax.experimental import pallas as pl
from jax.experimental.pallas import tpu as pltpu
from jax.sharding import PartitionSpec as P

F32, BF16 = jnp.float32, jnp.bfloat16
NT = (((1,), (1,)), ((), ()))
TN = (((0,), (0,)), ((), ()))
VMEM_LIMIT = 60 * 2**20
TILE = 512
COLS = 256
SMALL = 256
SLOTS = 6
LAYERS = (1, 0, 0, 0, 1, 1)
EVENTS = {
    0: (("greet",), ("own", 0), ("neighbours", 0), ("own", 1), ("opposite", 0), ("own", 2), ("relay", 0), ("complete", 0)),
    1: (("neighbours", 1),),
    2: (("own", 3),),
    4: (("neighbours", 2),),
    5: (("opposite", 1), ("own", 4)),
    7: (("relay", 1),),
    8: (("complete", 1), ("neighbours", 3)),
    9: (("opposite", 2), ("own", 5)),
    12: (("relay", 2),),
    13: (("neighbours", 4),),
    15: (("opposite", 3),),
    16: (("relay", 3), ("complete", 2), ("complete", 3)),
    17: (("neighbours", 5), ("opposite", 4)),
    18: (("relay", 4), ("opposite", 5)),
    19: (("complete", 4), ("relay", 5)),
    20: (("complete", 5),),
}


def dot(a, b):
    return jnp.dot(a, b, preferred_element_type=F32)


def dot_as(a, b, dims):
    return lax.dot_general(a, b, dims, preferred_element_type=F32)


def normed(h):
    wide = h.astype(F32)
    scale = lax.rsqrt(jnp.mean(wide * wide, -1, keepdims=True) + 1e-6)
    return wide, scale


def cuts(n, size):
    return [slice(at, min(at + size, n)) for at in range(0, n, size)]


def whole(shape):
    return pl.BlockSpec(shape, lambda *_: (0,) * len(shape), pipeline_mode=pl.Buffered(1))


def rows_of(width, tile=TILE):
    return pl.BlockSpec((tile, width), lambda i: (i, 0))


def params(**more):
    return pltpu.CompilerParams(dimension_semantics=("arbitrary",), vmem_limit_bytes=VMEM_LIMIT, **more)


def cost(matmuls, rows, d, ff, moved):
    return pl.CostEstimate(flops=2 * matmuls * rows * d * ff, bytes_accessed=moved, transcendentals=0)


class Gather:
    def __init__(self, n, shards, fulls, send, recv, local):
        self.n, self.shards, self.fulls, self.send, self.recv, self.local = n, shards, fulls, send, recv, local
        self.me = lax.axis_index("dp")
        rep = lax.axis_index("rep")
        core, chip = lax.rem(rep, 2), lax.rem(rep // 2, 2)
        self.outer = core == chip
        self.middle = core != chip
        self.bring, self.given, self.far = chip + core, chip + 1 - core, 2 - 2 * chip
        self.partner = {"rep": rep + 1 - 2 * core}
        self.twin = {"rep": rep + 2 - 4 * chip}
        self.right = {"dp": lax.rem(self.me + 1, n)}
        self.left = {"dp": lax.rem(self.me + n - 1, n)}

    def shard(self, m):
        return self.shards[m % 3].at[LAYERS[m]]

    def third(self, m, ref, row, which, part):
        block, width = self.shards[m % 3].shape[1:]
        if block % 6 == 0:
            rows = block // 3
            start, count = (0, rows) if part is None else (part * (rows // 2), rows // 2)
            return ref.at[pl.ds(pl.multiple_of(row + which * rows + start, 16), count)]
        columns = pl.ds(pl.multiple_of(which * (width // 3), 128), width // 3)
        start, count = (0, block) if part is None else (part * (block // 2), block // 2)
        return ref.at[pl.ds(pl.multiple_of(row + start, 16), count), columns]

    def piece(self, m, which, away, part=None):
        block = self.shards[m % 3].shape[1]
        return self.third(m, self.fulls[m], lax.rem(self.me + away + self.n, self.n) * block, which, part)

    def copy(self, m, k, src, dst, to):
        return pltpu.make_async_remote_copy(
            src_ref=src, dst_ref=dst, send_sem=self.send.at[m, k], recv_sem=self.recv.at[m, k],
            device_id=to, device_id_type=pl.DeviceIdType.MESH,
        )

    ARRIVALS = ((-1, None), (1, None), (2, 0), (2, 1))

    def ring(self, m, k):
        to = (self.right, self.left)[k % 2]
        if k < 2:
            return self.copy(m, k, self.third(m, self.shard(m), 0, self.bring, None), self.piece(m, self.bring, 0), to)
        ref = self.piece(m, self.bring, *((-1, 0), (1, 1))[k - 2])
        return self.copy(m, k, ref, ref, to)

    def hand(self, m, e, which, k, to):
        ref = self.piece(m, which, *self.ARRIVALS[e])
        return self.copy(m, k + e, ref, ref, to)

    def mine(self, m):
        block = self.shards[m % 3].shape[1]
        return pltpu.make_async_copy(self.shard(m), self.fulls[m].at[pl.ds(self.me * block, block)], self.local.at[m])

    def greet(self):
        barrier = pltpu.get_barrier_semaphore()
        for other in (self.left, self.right, self.partner, self.twin):
            pl.semaphore_signal(barrier, inc=1, device_id=other, device_id_type=pl.DeviceIdType.MESH)
        pl.semaphore_wait(barrier, 4)

    def own(self, m):
        for k in range(2):
            self.ring(m, k).start()
        self.mine(m).start()

    def arrived(self, m, e):
        self.hand(m, e, self.bring, 0, self.partner).wait_recv()
        if e < 2:
            self.ring(m, 2 + e).start()
        self.hand(m, e, self.bring, 4, self.partner).start()

        @pl.when(self.outer)
        def _():
            self.hand(m, e, self.bring, 8, self.twin).start()

    def neighbours(self, m):
        self.arrived(m, 0)
        self.arrived(m, 1)

    def opposite(self, m):
        self.arrived(m, 2)
        self.arrived(m, 3)

    def relay(self, m):
        @pl.when(self.middle)
        def _():
            for e in range(4):
                self.hand(m, e, self.far, 8, self.partner).wait_recv()
                self.hand(m, e, self.far, 8, self.partner).start()

    def complete(self, m):
        self.mine(m).wait()
        for e in range(4):
            self.hand(m, e, self.given, 4, self.partner).wait_recv()

        @pl.when(self.outer)
        def _():
            for e in range(4):
                self.hand(m, e, self.far, 8, self.partner).wait_recv()

    def sent(self, m):
        for k in range(4):
            self.ring(m, k).wait_send()
        for e in range(4):
            self.hand(m, e, self.bring, 4, self.partner).wait_send()
            self.hand(m, e, self.bring, 8, self.partner).wait_send()


def forward_kernel(n, x, dy, sd, sg, su, h1, a_out, acts, u_out, g_out, *rest):
    outs, fulls, (g_all, send, recv, local, out_sem, g_sem) = rest[:5], rest[5:11], rest[11:]
    gather = Gather(n, (sd, sg, su), fulls, send, recv, local)
    step = pl.program_id(0)
    tiles = pl.num_programs(0) // 3

    def keep(m):
        return pltpu.make_async_copy(fulls[m], outs[m - 1], out_sem.at[m - 1])

    def complete(m):
        gather.complete(m)
        if m:
            keep(m).start()

    for at, events in EVENTS.items():
        @pl.when(step == at)
        def _():
            for stage, *m in events:
                (complete if stage == "complete" else getattr(gather, stage))(*m)

    wd1, wg, wu, wd = fulls[:4]
    tile, ff = x.shape[0], wg.shape[1]

    def rows(t):
        return pl.ds(pl.multiple_of(t * tile, tile), tile)

    def keep_gate(t):
        return pltpu.make_async_copy(g_all.at[rows(t)], g_out.at[rows(t)], g_sem.at[t])

    @pl.when(step < tiles)
    def _():
        for s in cuts(ff, COLS):
            acts[0, :, s] = dot_as(dy[...], wd1[s, :], NT).astype(BF16)

    @pl.when((step >= tiles) & (step < 2 * tiles))
    def _():
        wide, scale = normed(x[...])
        a = (wide * scale).astype(BF16)
        a_out[...] = a
        for s in cuts(ff, COLS):
            g_all[rows(step - tiles), s] = dot(a, wg[:, s])
        keep_gate(step - tiles).start()

    @pl.when(step >= 2 * tiles)
    def _():
        h = x[...]
        wide, scale = normed(h)
        a = (wide * scale).astype(BF16)
        for s in cuts(ff, COLS):
            u = dot(a, wu[:, s])
            g = g_all[rows(step - 2 * tiles), s]
            u_out[:, s] = u
            acts[0, :, s] = (g * jax.nn.sigmoid(g) * u).astype(BF16)
        h1[...] = h + dot(acts[0], wd[...]).astype(BF16)

    @pl.when(step == pl.num_programs(0) - 1)
    def _():
        for m in range(6):
            gather.sent(m)
            if m:
                keep(m).wait()
        for t in range(8):
            keep_gate(t).wait()


def forward(n, x, dy, sg, su, sd):
    rows, d = x.shape
    ff = sg.shape[2]
    shapes = [(ff, d), (d, ff), (d, ff)] * 2
    tiles = rows // TILE
    assert tiles == 8 and n == 4
    outs = [((rows, d), BF16), ((rows, d), BF16), ((2, rows, ff), BF16), ((rows, ff), F32), ((rows, ff), F32)] + [(s, BF16) for s in shapes[1:]]
    anywhere = pl.BlockSpec(memory_space=pl.ANY)
    late = lambda width: pl.BlockSpec((TILE, width), lambda i: (jnp.maximum(i - 2 * tiles, 0), 0))
    dma = pltpu.SemaphoreType.DMA

    def acts_at(i):
        return jnp.where(i < 2 * tiles, 0, 1), jnp.where(i < 2 * tiles, jnp.minimum(i, tiles - 1), i - 2 * tiles), 0

    return pl.pallas_call(
        functools.partial(forward_kernel, n),
        grid=(3 * tiles,),
        out_shape=[jax.ShapeDtypeStruct(*o) for o in outs],
        in_specs=[
            pl.BlockSpec((TILE, d), lambda i: (lax.rem(i, tiles), 0)),
            pl.BlockSpec((TILE, d), lambda i: (jnp.minimum(i, tiles - 1), 0)),
        ]
        + [anywhere] * 3,
        out_specs=[
            late(d),
            pl.BlockSpec((TILE, d), lambda i: (jnp.clip(i - tiles, 0, tiles - 1), 0)),
            pl.BlockSpec((1, TILE, ff), acts_at),
            late(ff),
        ]
        + [anywhere] * 6,
        scratch_shapes=[pltpu.VMEM(s, BF16) for s in shapes]
        + [pltpu.VMEM((rows, ff), F32), dma((6, 12)), dma((6, 12)), dma((6,)), dma((5,)), dma((tiles,))],
        compiler_params=pltpu.CompilerParams(
            dimension_semantics=("arbitrary",), vmem_limit_bytes=67043328, collective_id=0, has_side_effects=True
        ),
        cost_estimate=cost(4, rows, d, ff, 130 * 2**20),
        name="forward",
    )(x, dy, sd, sg, su)


def through_norm(wide, scale, da, dh):
    m = jnp.mean(da * wide, -1, keepdims=True)
    return dh + (scale * da - wide * (scale * scale * scale * m)).astype(BF16)


def gate_grads(g, u, dact):
    sig = jax.nn.sigmoid(g)
    silu = g * sig
    return silu, (dact * u * (sig + silu * (1 - sig))).astype(BF16), (dact * silu).astype(BF16)


def last_kernel(h_ref, dy_ref, dacts, wg, wu, dh, a_out, act, dg, du):
    wide, scale = normed(h_ref[...])
    a = (wide * scale).astype(BF16)
    a_out[...] = a
    for s in cuts(wg.shape[1], COLS):
        g = dot(a, wg[:, s])
        u = dot(a, wu[:, s])
        silu, dg[:, s], du[:, s] = gate_grads(g, u, dacts[0, :, s].astype(F32))
        act[:, s] = (silu * u).astype(BF16)
    da = dot_as(dg[...], wg[...], NT) + dot_as(du[...], wu[...], NT)
    dh[...] = through_norm(wide, scale, da.astype(BF16).astype(F32), dy_ref[...])


def last(h, dy, acts, wg, wu):
    rows, d = h.shape
    ff = wg.shape[1]
    return pl.pallas_call(
        last_kernel,
        grid=(rows // TILE,),
        out_shape=[jax.ShapeDtypeStruct((rows, d), BF16)] * 2 + [jax.ShapeDtypeStruct((rows, ff), BF16)] * 3,
        in_specs=[rows_of(d), rows_of(d), pl.BlockSpec((1, TILE, ff), lambda i: (0, i, 0))] + [whole(w.shape) for w in (wg, wu)],
        out_specs=[rows_of(d)] * 2 + [rows_of(ff)] * 3,
        compiler_params=params(),
        cost_estimate=cost(4, rows, d, ff, 90 * 2**20),
        name="last",
    )(h, dy, acts, wg, wu)


class Scatter:
    def __init__(self, n, rows, keep, s1, r1, s2, r2, send, recv):
        self.rows, self.keep, self.s1, self.r1, self.s2, self.r2, self.send, self.recv = rows, keep, s1, r1, s2, r2, send, recv
        self.n = n
        self.me = lax.axis_index("dp")
        self.right = {"dp": lax.rem(self.me + 1, n)}
        self.left = {"dp": lax.rem(self.me + n - 1, n)}

    def copy(self, slot, k, src, dst):
        return pltpu.make_async_remote_copy(
            src_ref=src, dst_ref=dst, send_sem=self.send.at[slot, k], recv_sem=self.recv.at[slot, k],
            device_id=self.left if k % 2 else self.right, device_id_type=pl.DeviceIdType.MESH,
        )

    def opposites(self, slot, k):
        half = self.rows // 2
        return self.copy(slot, k, self.s1.at[slot, pl.ds(k * half, half)], self.r1.at[slot, k])

    def sums(self, slot, k):
        return self.copy(slot, 2 + k, self.s2.at[slot, k], self.r2.at[slot, k])

    def of(self, term, away):
        at = pl.multiple_of(lax.rem(self.me + away, self.n) * self.rows, 64)
        return term[pl.ds(at, self.rows), :]

    def put(self, slot, term):
        self.s1[slot] = self.of(term, 2).astype(BF16)
        self.keep[slot, 0] = self.of(term, 1)
        self.keep[slot, 1] = self.of(term, self.n - 1)
        self.keep[slot, 2] = self.of(term, 0)

    def begin(self, slot):
        for k in range(2):
            self.opposites(slot, k).start()

    def middle(self, slot):
        half = self.rows // 2
        for k in range(2):
            self.opposites(slot, k).wait_recv()
        for k in range(2):
            with_theirs, alone = pl.ds(k * half, half), pl.ds((1 - k) * half, half)
            self.s2[slot, k, with_theirs] = (self.keep[slot, k, with_theirs] + self.r1[slot, k].astype(F32)).astype(BF16)
            self.s2[slot, k, alone] = self.keep[slot, k, alone].astype(BF16)
        for k in range(2):
            self.sums(slot, k).start()

    def end(self, slot):
        for k in range(2):
            self.sums(slot, k).wait_recv()
        out = self.keep[slot, 2] + self.r2[slot, 0].astype(F32) + self.r2[slot, 1].astype(F32)
        for k in range(2):
            self.opposites(slot, k).wait_send()
            self.sums(slot, k).wait_send()
        return out.astype(BF16)


def backward_kernel(
    n, dims, dy, dh1, x, a0, a1, acts, act1, dg1, du1, g0, u0, wg0, wu0, wd0,
    wide_out, down_out, dx, dg0, du0,
    ra, ract, blk, term, wd, g_t, u_t, dh_t, dg_t, du_t, x_t, dx_t,
    wk, ws1, wr1, ws2, wr2, dk, ds1, dr1, ds2, dr2,
    wsend, wrecv, dsend, drecv, blk_sem, res_sem, in_sem, out_sem,
):
    rows, d, ff = dims
    tiles = rows // SMALL
    wides, downs = ff // COLS, d // COLS
    first_tiles = tiles // 2 - downs
    wide = Scatter(n, d // n, wk, ws1, wr1, ws2, wr2, wsend, wrecv)
    down = Scatter(n, ff // n, dk, ds1, dr1, ds2, dr2, dsend, drecv)

    def resident(src, dst, k):
        return pltpu.make_async_copy(src, dst, res_sem.at[k])

    load_a1 = lambda: resident(a1, ra, 0)
    load_a0 = lambda: resident(a0, ra, 0)
    load_act1 = lambda: resident(act1, ract, 1)
    load_act0 = lambda: resident(acts.at[1], ract, 1)
    load_wd = lambda: resident(wd0, wd, 2)
    load_wg = lambda: resident(wg0, ract.at[pl.ds(0, d)], 1)
    load_wu = lambda: resident(wu0, ract.at[pl.ds(d, d)], 2)

    def column(src, j, slot):
        return pltpu.make_async_copy(src.at[:, pl.ds(pl.multiple_of(j * COLS, COLS), COLS)], blk.at[slot], blk_sem.at[slot])

    def load_wide(r, i, slot):
        for at, src in ((0, dg1), (1, du1)):
            @pl.when(r == at)
            def _():
                column(src, i, slot).start()

    def load_down(r, j, slot):
        for at, src in ((0, dy), (1, dh1)):
            @pl.when(r == at)
            def _():
                column(src, j, slot).start()

    def load_last(i, slot):
        @pl.when(i < wides)
        def _():
            column(dg0, i, slot).start()

        @pl.when(i >= wides)
        def _():
            column(du0, i - wides, slot).start()

    def tile_of(ref, t):
        return ref.at[pl.ds(pl.multiple_of(t * SMALL, SMALL), SMALL)]

    def tile_in(t):
        slot = lax.rem(t, 2)
        return [pltpu.make_async_copy(tile_of(src, t), dst.at[slot], in_sem.at[k, slot]) for k, (src, dst) in enumerate(((g0, g_t), (u0, u_t), (dh1, dh_t)))]

    def tile_out(t):
        slot = lax.rem(t, 2)
        return [pltpu.make_async_copy(src.at[slot], tile_of(dst, t), out_sem.at[k, slot]) for k, (src, dst) in enumerate(((dg_t, dg0), (du_t, du0)))]

    def tile(t):
        slot = lax.rem(t, 2)
        for c in tile_in(t):
            c.wait()

        @pl.when(t + 1 < tiles)
        def _():
            for c in tile_in(t + 1):
                c.start()

        @pl.when(t >= 2)
        def _():
            for c in tile_out(t - 2):
                c.wait()

        dh = dh_t[slot]
        for s in cuts(ff, COLS):
            dact = dot_as(dh, wd[s, :], NT).astype(BF16).astype(F32)
            _, dg_t[slot, :, s], du_t[slot, :, s] = gate_grads(g_t[slot, :, s], u_t[slot, :, s], dact)
        for c in tile_out(t):
            c.start()

    def late_in(t):
        slot = lax.rem(t, 2)
        pairs = ((dg0, dg_t), (du0, du_t), (dh1, dh_t), (x, x_t))
        return [pltpu.make_async_copy(tile_of(src, t), dst.at[slot], in_sem.at[k, slot]) for k, (src, dst) in enumerate(pairs)]

    def late_out(t):
        slot = lax.rem(t, 2)
        return pltpu.make_async_copy(dx_t.at[slot], tile_of(dx, t), out_sem.at[0, slot])

    def late(t):
        slot = lax.rem(t, 2)
        for c in late_in(t):
            c.wait()

        @pl.when(t + 1 < tiles)
        def _():
            for c in late_in(t + 1):
                c.start()

        @pl.when(t >= 2)
        def _():
            late_out(t - 2).wait()

        h, scale = normed(x_t[slot])
        da = dot_as(dg_t[slot], ract[0:d, :], NT) + dot_as(du_t[slot], ract[d : 2 * d, :], NT)
        dx_t[slot] = through_norm(h, scale, da.astype(BF16).astype(F32), dh_t[slot])
        late_out(t).start()

    def end_wide(k):
        wide_out[k // wides, :, pl.ds(pl.multiple_of(lax.rem(k, wides) * COLS, COLS), COLS)] = wide.end(lax.rem(k, SLOTS))

    def end_down(r, j):
        down_out[r, :, pl.ds(pl.multiple_of(j * COLS, COLS), COLS)] = down.end(j)

    def due_wide(r, i):
        k = wides * r + i

        @pl.when(i >= 2)
        def _():
            wide.middle(lax.rem(k + SLOTS - 2, SLOTS))

        @pl.when((r >= 1) & (i < 2))
        def _():
            down.middle(i + downs - 2)

        @pl.when(i >= 4)
        def _():
            end_wide(k - 4)

        @pl.when((r >= 1) & (i == 0))
        def _():
            end_wide(k - 1)

        @pl.when((r >= 1) & (i >= 1) & (i < 4))
        def _():
            end_down(r - 1, i - 1)

    def due_down(r, j):
        k = wides * r + wides + j

        @pl.when(j < 2)
        def _():
            wide.middle(lax.rem(k - 2, SLOTS))

        @pl.when(j == 2)
        def _():
            down.middle(0)

        end_wide(k - 4)

    def wide_step(r, i, slot, tail):
        term[0:d, :] = dot_as(ra[...], blk[slot], TN)
        k = lax.rem(wides * r + i, SLOTS)
        wide.put(k, term)
        due_wide(r, i)
        tail()
        wide.begin(k)

    load_a1().start()
    load_wide(0, 0, 0)
    load_wd().start()
    for c in tile_in(0):
        c.start()
    load_act1().start()
    barrier = pltpu.get_barrier_semaphore()
    for other in (wide.left, wide.right):
        pl.semaphore_signal(barrier, inc=1, device_id=other, device_id_type=pl.DeviceIdType.MESH)
    pl.semaphore_wait(barrier, 2)
    load_a1().wait()
    load_wd().wait()

    def round_(r, _):
        def wide_block(i, _):
            q = (wides + downs) * r + i
            slot = lax.rem(q, 2)
            column(dg1, 0, slot).wait()

            @pl.when(i + 1 < wides)
            def _():
                load_wide(r, i + 1, 1 - slot)

            @pl.when(i + 1 == wides)
            def _():
                load_down(r, 0, 1 - slot)

            def tail():
                at = (i * first_tiles) // wides

                @pl.when(((i + 1) * first_tiles) // wides > at)
                def _():
                    tile(r * (tiles // 2) + at)

            wide_step(r, i, slot, tail)
            return 0

        lax.fori_loop(0, wides, wide_block, 0)

        @pl.when(r == 1)
        def _():
            load_a0().start()

        load_act1().wait()

        def down_block(j, _):
            q = (wides + downs) * r + wides + j
            slot = lax.rem(q, 2)
            column(dy, 0, slot).wait()

            @pl.when(j + 1 < downs)
            def _():
                load_down(r, j + 1, 1 - slot)

            @pl.when((j + 1 == downs) & (r == 0))
            def _():
                load_wide(r + 1, 0, 1 - slot)

            for s in cuts(ff, ff // 2):
                term[s, :] = dot_as(ract[:, s], blk[slot], TN)
            down.put(j, term)
            due_down(r, j)
            tile(r * (tiles // 2) + first_tiles + j)
            down.begin(j)
            return 0

        lax.fori_loop(0, downs, down_block, 0)

        @pl.when(r == 0)
        def _():
            load_act0().start()

        return 0

    lax.fori_loop(0, 2, round_, 0)

    for t in (tiles - 2, tiles - 1):
        for c in tile_out(t):
            c.wait()
    last_q = 2 * (wides + downs)
    load_last(0, last_q % 2)
    load_wg().start()
    load_wu().start()
    for c in late_in(0):
        c.start()
    load_a0().wait()
    load_wg().wait()
    load_wu().wait()
    blocks = 2 * wides
    late_early = tiles // 2

    def last_block(i, _):
        slot = lax.rem(last_q + i, 2)
        column(dg0, 0, slot).wait()

        @pl.when(i + 1 < blocks)
        def _():
            load_last(i + 1, 1 - slot)

        def tail():
            at = (i * late_early) // blocks

            @pl.when(((i + 1) * late_early) // blocks > at)
            def _():
                late(at)

        wide_step(2, i, slot, tail)
        return 0

    lax.fori_loop(0, blocks, last_block, 0)

    def rest(v, _):
        k = 2 * wides + blocks + v

        def pair(p, _):
            late(late_early + 2 * v + p)
            return 0

        lax.fori_loop(0, 2, pair, 0)

        @pl.when(v < 2)
        def _():
            wide.middle(lax.rem(k - 2, SLOTS))

        end_wide(k - 4)
        return 0

    lax.fori_loop(0, 4, rest, 0)
    for t in (tiles - 2, tiles - 1):
        late_out(t).wait()


def backward(n, dy, dh1, x, a0, a1, acts, act1, dg1, du1, g0, u0, wg0, wu0, wd0):
    rows, d = dy.shape
    ff = act1.shape[1]
    wide, down = d // n, ff // n
    assert n == 4 and rows // SMALL == 16 and d == 3 * COLS and ff == 7 * COLS
    anywhere = pl.BlockSpec(memory_space=pl.ANY)
    inside = pl.BlockSpec(memory_space=pltpu.VMEM)

    def slots(count, chunk):
        return [
            pltpu.VMEM((count, 3, chunk, COLS), F32),
            pltpu.VMEM((count, chunk, COLS), BF16),
            pltpu.VMEM((count, 2, chunk // 2, COLS), BF16),
            pltpu.VMEM((count, 2, chunk, COLS), BF16),
            pltpu.VMEM((count, 2, chunk, COLS), BF16),
        ]

    dma = pltpu.SemaphoreType.DMA
    return pl.pallas_call(
        functools.partial(backward_kernel, n, (rows, d, ff)),
        out_shape=[
            jax.ShapeDtypeStruct((4, wide, ff), BF16),
            jax.ShapeDtypeStruct((2, down, d), BF16),
            jax.ShapeDtypeStruct((rows, d), BF16),
            jax.ShapeDtypeStruct((rows, ff), BF16),
            jax.ShapeDtypeStruct((rows, ff), BF16),
        ],
        in_specs=[anywhere] * 14,
        out_specs=[inside, inside, anywhere, anywhere, anywhere],
        scratch_shapes=[
            pltpu.VMEM((rows, d), BF16),
            pltpu.VMEM((rows, ff), BF16),
            pltpu.VMEM((2, rows, COLS), BF16),
            pltpu.VMEM((ff, COLS), F32),
            pltpu.VMEM((ff, d), BF16),
            pltpu.VMEM((2, SMALL, ff), F32),
            pltpu.VMEM((2, SMALL, ff), F32),
            pltpu.VMEM((2, SMALL, d), BF16),
            pltpu.VMEM((2, SMALL, ff), BF16),
            pltpu.VMEM((2, SMALL, ff), BF16),
            pltpu.VMEM((2, SMALL, d), BF16),
            pltpu.VMEM((2, SMALL, d), BF16),
            *slots(SLOTS, wide),
            *slots(3, down),
            dma((SLOTS, 4)), dma((SLOTS, 4)), dma((3, 4)), dma((3, 4)),
            dma((2,)), dma((3,)), dma((4, 2)), dma((2, 2)),
        ],
        compiler_params=pltpu.CompilerParams(vmem_limit_bytes=67043328, collective_id=1, has_side_effects=True),
        cost_estimate=cost(9, rows, d, ff, 300 * 2**20),
        name="backward",
    )(dy, dh1, x, a0, a1, acts, act1, dg1, du1, g0, u0, wg0, wu0, wd0)


def solution(mesh):
    n = mesh.shape["dp"]

    def body(x, dy, sg, su, sd):
        x, dy = x[0], dy[0]
        h1, a0, acts, u0, g0, wg0, wu0, wd0, wg1, wu1 = forward(n, x, dy, sg, su, sd)
        dh1, a1, act1, dg1, du1 = last(h1, dy, acts, wg1, wu1)
        wide, down, dx, _, _ = backward(n, dy, dh1, x, a0, a1, acts, act1, dg1, du1, g0, u0, wg0, wu0, wd0)
        gate1, up1, gate0, up0 = wide
        down1, down0 = down
        return dx[None], jnp.stack([gate0, gate1]), jnp.stack([up0, up1]), jnp.stack([down0, down1])

    tokens = P(("rep", "dp"), None, None)
    return jax.shard_map(
        body,
        mesh=mesh,
        in_specs=(tokens, tokens) + (P(None, "dp", None),) * 3,
        out_specs=(tokens,) + (P("rep", "dp", None),) * 3,
        check_vma=False,
    )
```

```python
import functools

import jax
import jax.numpy as jnp
from jax import lax
from jax.experimental import pallas as pl
from jax.experimental.pallas import tpu as pltpu
from jax.sharding import PartitionSpec as P

F32, BF16 = jnp.float32, jnp.bfloat16
NT = (((1,), (1,)), ((), ()))
TN = (((0,), (0,)), ((), ()))
VMEM_LIMIT = 60 * 2**20
TILE = 512
COLS = 256
SMALL = 256
SLOTS = 9
ON, DONE = 4, 8
LAYERS = (1, 0, 0, 0, 1, 1)
EVENTS = {
    0: (
        ("greet",), ("own", 0), ("neighbours", 0), ("own", 1), ("opposite", 0), ("own", 2), ("relay", 0), ("neighbours", 1), ("own", 3), ("complete", 0),
    ),
    3: (("opposite", 1), ("neighbours", 2), ("own", 4)),
    5: (("relay", 1),),
    6: (("opposite", 2), ("neighbours", 3), ("own", 5)),
    8: (("complete", 1),),
    9: (("relay", 2),),
    10: (("opposite", 3),),
    12: (("neighbours", 4),),
    13: (("relay", 3),),
    14: (("opposite", 4), ("neighbours", 5)),
    16: (("complete", 2), ("complete", 3)),
    17: (("relay", 4), ("opposite", 5)),
    18: (("complete", 4),),
    19: (("relay", 5),),
    20: (("complete", 5),),
}


def dot(a, b):
    return jnp.dot(a, b, preferred_element_type=F32)


def dot_as(a, b, dims):
    return lax.dot_general(a, b, dims, preferred_element_type=F32)


def normed(h):
    wide = h.astype(F32)
    scale = lax.rsqrt(jnp.mean(wide * wide, -1, keepdims=True) + 1e-6)
    return wide, scale


def cuts(n, size):
    return [slice(at, min(at + size, n)) for at in range(0, n, size)]


def whole(shape):
    return pl.BlockSpec(shape, lambda *_: (0,) * len(shape), pipeline_mode=pl.Buffered(1))


def rows_of(width, tile=TILE):
    return pl.BlockSpec((tile, width), lambda i: (i, 0))


def params(**more):
    return pltpu.CompilerParams(dimension_semantics=("arbitrary",), vmem_limit_bytes=VMEM_LIMIT, **more)


def cost(matmuls, rows, d, ff, moved):
    return pl.CostEstimate(flops=2 * matmuls * rows * d * ff, bytes_accessed=moved, transcendentals=0)


class Gather:
    def __init__(self, n, shards, fulls, send, recv, local):
        self.n, self.shards, self.fulls, self.send, self.recv, self.local = n, shards, fulls, send, recv, local
        self.me = lax.axis_index("dp")
        rep = lax.axis_index("rep")
        core, chip = lax.rem(rep, 2), lax.rem(rep // 2, 2)
        self.outer = core == chip
        self.middle = core != chip
        self.bring, self.given, self.far = chip + core, chip + 1 - core, 2 - 2 * chip
        self.partner = {"rep": rep + 1 - 2 * core}
        self.twin = {"rep": rep + 2 - 4 * chip}
        self.right = {"dp": lax.rem(self.me + 1, n)}
        self.left = {"dp": lax.rem(self.me + n - 1, n)}

    def shard(self, m):
        return self.shards[m % 3].at[LAYERS[m]]

    def third(self, m, ref, row, which, part):
        block, width = self.shards[m % 3].shape[1:]
        if block % 6 == 0:
            rows = block // 3
            start, count = (0, rows) if part is None else (part * (rows // 2), rows // 2)
            return ref.at[pl.ds(pl.multiple_of(row + which * rows + start, 16), count)]
        columns = pl.ds(pl.multiple_of(which * (width // 3), 128), width // 3)
        start, count = (0, block) if part is None else (part * (block // 2), block // 2)
        return ref.at[pl.ds(pl.multiple_of(row + start, 16), count), columns]

    def piece(self, m, which, away, part=None):
        block = self.shards[m % 3].shape[1]
        return self.third(m, self.fulls[m], lax.rem(self.me + away + self.n, self.n) * block, which, part)

    def copy(self, m, k, src, dst, to):
        return pltpu.make_async_remote_copy(
            src_ref=src, dst_ref=dst, send_sem=self.send.at[m, k], recv_sem=self.recv.at[m, k],
            device_id=to, device_id_type=pl.DeviceIdType.MESH,
        )

    ARRIVALS = ((-1, None), (1, None), (2, 0), (2, 1))

    def ring(self, m, k):
        to = (self.right, self.left)[k % 2]
        if k < 2:
            return self.copy(m, k, self.third(m, self.shard(m), 0, self.bring, None), self.piece(m, self.bring, 0), to)
        ref = self.piece(m, self.bring, *((-1, 0), (1, 1))[k - 2])
        return self.copy(m, k, ref, ref, to)

    def hand(self, m, e, which, k, to):
        ref = self.piece(m, which, *self.ARRIVALS[e])
        return self.copy(m, k + e, ref, ref, to)

    def mine(self, m):
        block = self.shards[m % 3].shape[1]
        return pltpu.make_async_copy(self.shard(m), self.fulls[m].at[pl.ds(self.me * block, block)], self.local.at[m])

    def greet(self):
        barrier = pltpu.get_barrier_semaphore()
        for other in (self.left, self.right, self.partner, self.twin):
            pl.semaphore_signal(barrier, inc=1, device_id=other, device_id_type=pl.DeviceIdType.MESH)
        pl.semaphore_wait(barrier, 4)

    def own(self, m):
        for k in range(2):
            self.ring(m, k).start()
        self.mine(m).start()

    def arrived(self, m, e):
        self.hand(m, e, self.bring, 0, self.partner).wait_recv()
        if e < 2:
            self.ring(m, 2 + e).start()
        self.hand(m, e, self.bring, 4, self.partner).start()

        @pl.when(self.outer)
        def _():
            self.hand(m, e, self.bring, 8, self.twin).start()

    def neighbours(self, m):
        self.arrived(m, 0)
        self.arrived(m, 1)

    def opposite(self, m):
        self.arrived(m, 2)
        self.arrived(m, 3)

    def relay(self, m):
        @pl.when(self.middle)
        def _():
            for e in range(4):
                self.hand(m, e, self.far, 8, self.partner).wait_recv()
                self.hand(m, e, self.far, 8, self.partner).start()

    def complete(self, m):
        self.mine(m).wait()
        for e in range(4):
            self.hand(m, e, self.given, 4, self.partner).wait_recv()

        @pl.when(self.outer)
        def _():
            for e in range(4):
                self.hand(m, e, self.far, 8, self.partner).wait_recv()

    def sent(self, m):
        for k in range(4):
            self.ring(m, k).wait_send()
        for e in range(4):
            self.hand(m, e, self.bring, 4, self.partner).wait_send()
            self.hand(m, e, self.bring, 8, self.partner).wait_send()


def forward_kernel(n, x, dy, sd, sg, su, h1, a_out, acts, u_out, g_out, *rest):
    outs, fulls, (g_all, send, recv, local, out_sem, g_sem) = rest[:5], rest[5:11], rest[11:]
    gather = Gather(n, (sd, sg, su), fulls, send, recv, local)
    step = pl.program_id(0)
    tiles = pl.num_programs(0) // 3

    def keep(m):
        return pltpu.make_async_copy(fulls[m], outs[m - 1], out_sem.at[m - 1])

    def complete(m):
        gather.complete(m)
        if m:
            keep(m).start()

    for at, events in EVENTS.items():
        @pl.when(step == at)
        def _():
            for stage, *m in events:
                (complete if stage == "complete" else getattr(gather, stage))(*m)

    wd1, wg, wu, wd = fulls[:4]
    tile, ff = x.shape[0], wg.shape[1]

    def rows(t):
        return pl.ds(pl.multiple_of(t * tile, tile), tile)

    def keep_gate(t):
        return pltpu.make_async_copy(g_all.at[rows(t)], g_out.at[rows(t)], g_sem.at[t])

    @pl.when(step < tiles)
    def _():
        for s in cuts(ff, COLS):
            acts[0, :, s] = dot_as(dy[...], wd1[s, :], NT).astype(BF16)

    @pl.when((step >= tiles) & (step < 2 * tiles))
    def _():
        wide, scale = normed(x[...])
        a = (wide * scale).astype(BF16)
        a_out[...] = a
        for s in cuts(ff, COLS):
            g_all[rows(step - tiles), s] = dot(a, wg[:, s])
        keep_gate(step - tiles).start()

    @pl.when(step >= 2 * tiles)
    def _():
        h = x[...]
        wide, scale = normed(h)
        a = (wide * scale).astype(BF16)
        for s in cuts(ff, COLS):
            u = dot(a, wu[:, s])
            g = g_all[rows(step - 2 * tiles), s]
            u_out[:, s] = u
            acts[0, :, s] = (g * jax.nn.sigmoid(g) * u).astype(BF16)
        h1[...] = h + dot(acts[0], wd[...]).astype(BF16)

    @pl.when(step == pl.num_programs(0) - 1)
    def _():
        for m in range(6):
            gather.sent(m)
            if m:
                keep(m).wait()
        for t in range(8):
            keep_gate(t).wait()


def forward(n, x, dy, sg, su, sd):
    rows, d = x.shape
    ff = sg.shape[2]
    shapes = [(ff, d), (d, ff), (d, ff)] * 2
    tiles = rows // TILE
    assert tiles == 8 and n == 4
    outs = [((rows, d), BF16), ((rows, d), BF16), ((2, rows, ff), BF16), ((rows, ff), F32), ((rows, ff), F32)] + [(s, BF16) for s in shapes[1:]]
    anywhere = pl.BlockSpec(memory_space=pl.ANY)
    late = lambda width: pl.BlockSpec((TILE, width), lambda i: (jnp.maximum(i - 2 * tiles, 0), 0))
    dma = pltpu.SemaphoreType.DMA

    def acts_at(i):
        return jnp.where(i < 2 * tiles, 0, 1), jnp.where(i < 2 * tiles, jnp.minimum(i, tiles - 1), i - 2 * tiles), 0

    return pl.pallas_call(
        functools.partial(forward_kernel, n),
        grid=(3 * tiles,),
        out_shape=[jax.ShapeDtypeStruct(*o) for o in outs],
        in_specs=[
            pl.BlockSpec((TILE, d), lambda i: (lax.rem(i, tiles), 0)),
            pl.BlockSpec((TILE, d), lambda i: (jnp.minimum(i, tiles - 1), 0)),
        ]
        + [anywhere] * 3,
        out_specs=[
            late(d),
            pl.BlockSpec((TILE, d), lambda i: (jnp.clip(i - tiles, 0, tiles - 1), 0)),
            pl.BlockSpec((1, TILE, ff), acts_at),
            late(ff),
        ]
        + [anywhere] * 6,
        scratch_shapes=[pltpu.VMEM(s, BF16) for s in shapes]
        + [pltpu.VMEM((rows, ff), F32), dma((6, 12)), dma((6, 12)), dma((6,)), dma((5,)), dma((tiles,))],
        compiler_params=pltpu.CompilerParams(
            dimension_semantics=("arbitrary",), vmem_limit_bytes=67043328, collective_id=0, has_side_effects=True
        ),
        cost_estimate=cost(4, rows, d, ff, 130 * 2**20),
        name="forward",
    )(x, dy, sd, sg, su)


def through_norm(wide, scale, da, dh):
    m = jnp.mean(da * wide, -1, keepdims=True)
    return dh + (scale * da - wide * (scale * scale * scale * m)).astype(BF16)


def gate_grads(g, u, dact):
    sig = jax.nn.sigmoid(g)
    silu = g * sig
    return silu, (dact * u * (sig + silu * (1 - sig))).astype(BF16), (dact * silu).astype(BF16)


def last_kernel(h_ref, dy_ref, dacts, wg, wu, dh, a_out, act, dg, du):
    wide, scale = normed(h_ref[...])
    a = (wide * scale).astype(BF16)
    a_out[...] = a
    for s in cuts(wg.shape[1], COLS):
        g = dot(a, wg[:, s])
        u = dot(a, wu[:, s])
        silu, dg[:, s], du[:, s] = gate_grads(g, u, dacts[0, :, s].astype(F32))
        act[:, s] = (silu * u).astype(BF16)
    da = dot_as(dg[...], wg[...], NT) + dot_as(du[...], wu[...], NT)
    dh[...] = through_norm(wide, scale, da.astype(BF16).astype(F32), dy_ref[...])


def last(h, dy, acts, wg, wu):
    rows, d = h.shape
    ff = wg.shape[1]
    return pl.pallas_call(
        last_kernel,
        grid=(rows // TILE,),
        out_shape=[jax.ShapeDtypeStruct((rows, d), BF16)] * 2 + [jax.ShapeDtypeStruct((rows, ff), BF16)] * 3,
        in_specs=[rows_of(d), rows_of(d), pl.BlockSpec((1, TILE, ff), lambda i: (0, i, 0))] + [whole(w.shape) for w in (wg, wu)],
        out_specs=[rows_of(d)] * 2 + [rows_of(ff)] * 3,
        compiler_params=params(),
        cost_estimate=cost(4, rows, d, ff, 90 * 2**20),
        name="last",
    )(h, dy, acts, wg, wu)


class Scatter:
    def __init__(self, n, rows, keep, s1, r1, s2, r2, send, recv):
        self.rows, self.keep, self.s1, self.r1, self.s2, self.r2, self.send, self.recv = rows, keep, s1, r1, s2, r2, send, recv
        self.n = n
        self.me = lax.axis_index("dp")
        self.right = {"dp": lax.rem(self.me + 1, n)}
        self.left = {"dp": lax.rem(self.me + n - 1, n)}

    def copy(self, slot, k, src, dst):
        return pltpu.make_async_remote_copy(
            src_ref=src, dst_ref=dst, send_sem=self.send.at[slot, k], recv_sem=self.recv.at[slot, k],
            device_id=self.left if k % 2 else self.right, device_id_type=pl.DeviceIdType.MESH,
        )

    def opposites(self, slot, k):
        half = self.rows // 2
        return self.copy(slot, k, self.s1.at[slot, pl.ds(k * half, half)], self.r1.at[slot, k])

    def sums(self, slot, k):
        return self.copy(slot, 2 + k, self.s2.at[slot, k], self.r2.at[slot, k])

    def of(self, term, away):
        at = pl.multiple_of(lax.rem(self.me + away, self.n) * self.rows, 64)
        return term[pl.ds(at, self.rows), :]

    def put(self, slot, term):
        self.s1[slot] = self.of(term, 2).astype(BF16)
        self.keep[slot, 0] = self.of(term, 1)
        self.keep[slot, 1] = self.of(term, self.n - 1)
        self.keep[slot, 2] = self.of(term, 0)

    def begin(self, slot):
        for k in range(2):
            self.opposites(slot, k).start()

    def middle(self, slot):
        half = self.rows // 2
        for k in range(2):
            self.opposites(slot, k).wait_recv()
        for k in range(2):
            with_theirs, alone = pl.ds(k * half, half), pl.ds((1 - k) * half, half)
            self.s2[slot, k, with_theirs] = (self.keep[slot, k, with_theirs] + self.r1[slot, k].astype(F32)).astype(BF16)
            self.s2[slot, k, alone] = self.keep[slot, k, alone].astype(BF16)
        for k in range(2):
            self.sums(slot, k).start()

    def end(self, slot):
        for k in range(2):
            self.sums(slot, k).wait_recv()
        out = self.keep[slot, 2] + self.r2[slot, 0].astype(F32) + self.r2[slot, 1].astype(F32)
        for k in range(2):
            self.opposites(slot, k).wait_send()
            self.sums(slot, k).wait_send()
        return out.astype(BF16)


def backward_kernel(
    n, dims, dy, dh1, x, a0, a1, acts, act1, dg1, du1, g0, u0, wg0, wu0, wd0,
    wide_out, down_out, dx, dg0, du0,
    ra, ract, blk, term, wd, g_t, u_t, dh_t, dg_t, du_t, x_t, dx_t,
    wk, ws1, wr1, ws2, wr2, dk, ds1, dr1, ds2, dr2,
    wsend, wrecv, dsend, drecv, blk_sem, res_sem, in_sem, out_sem,
):
    rows, d, ff = dims
    tiles = rows // SMALL
    wides, downs = ff // COLS, d // COLS
    first_tiles = tiles // 2 - downs + 1
    wide = Scatter(n, d // n, wk, ws1, wr1, ws2, wr2, wsend, wrecv)
    down = Scatter(n, ff // n, dk, ds1, dr1, ds2, dr2, dsend, drecv)

    def resident(src, dst, k):
        return pltpu.make_async_copy(src, dst, res_sem.at[k])

    load_a1 = lambda: resident(a1, ra, 0)
    load_a0 = lambda: resident(a0, ra, 0)
    load_act1 = lambda: resident(act1, ract, 1)
    load_act0 = lambda: resident(acts.at[1], ract, 1)
    load_wd = lambda: resident(wd0, wd, 2)
    load_wg = lambda: resident(wg0, ract.at[pl.ds(0, d)], 1)
    load_wu = lambda: resident(wu0, ract.at[pl.ds(d, d)], 2)

    def column(src, j, slot):
        return pltpu.make_async_copy(src.at[:, pl.ds(pl.multiple_of(j * COLS, COLS), COLS)], blk.at[slot], blk_sem.at[slot])

    def load_wide(r, i, slot):
        for at, src in ((0, dg1), (1, du1)):
            @pl.when(r == at)
            def _():
                column(src, i, slot).start()

    def load_down(r, j, slot):
        for at, src in ((0, dy), (1, dh1)):
            @pl.when(r == at)
            def _():
                column(src, j, slot).start()

    def load_last(i, slot):
        @pl.when(i < wides)
        def _():
            column(dg0, i, slot).start()

        @pl.when(i >= wides)
        def _():
            column(du0, i - wides, slot).start()

    def tile_of(ref, t):
        return ref.at[pl.ds(pl.multiple_of(t * SMALL, SMALL), SMALL)]

    def tile_in(t):
        pairs = ((g0, g_t), (u0, u_t), (dh1, dh_t.at[0]))
        return [pltpu.make_async_copy(tile_of(src, t), dst, in_sem.at[k, 0]) for k, (src, dst) in enumerate(pairs)]

    def tile_out(t):
        slot = lax.rem(t, 2)
        return [pltpu.make_async_copy(src.at[slot], tile_of(dst, t), out_sem.at[k, slot]) for k, (src, dst) in enumerate(((dg_t, dg0), (du_t, du0)))]

    def tile(t):
        slot = lax.rem(t, 2)
        for c in tile_in(t):
            c.wait()

        @pl.when(t >= 2)
        def _():
            for c in tile_out(t - 2):
                c.wait()

        dh = dh_t[0]
        for s in cuts(ff, COLS):
            dact = dot_as(dh, wd[s, :], NT).astype(BF16).astype(F32)
            _, dg_t[slot, :, s], du_t[slot, :, s] = gate_grads(g_t[:, s], u_t[:, s], dact)

        @pl.when(t + 1 < tiles)
        def _():
            for c in tile_in(t + 1):
                c.start()

        for c in tile_out(t):
            c.start()

    def late_in(t):
        slot = lax.rem(t, 2)
        pairs = ((dg0, dg_t), (du0, du_t), (dh1, dh_t), (x, x_t))
        return [pltpu.make_async_copy(tile_of(src, t), dst.at[slot], in_sem.at[k, slot]) for k, (src, dst) in enumerate(pairs)]

    def late_out(t):
        slot = lax.rem(t, 2)
        return pltpu.make_async_copy(dx_t.at[slot], tile_of(dx, t), out_sem.at[0, slot])

    def late(t):
        slot = lax.rem(t, 2)
        for c in late_in(t):
            c.wait()

        @pl.when(t + 1 < tiles)
        def _():
            for c in late_in(t + 1):
                c.start()

        @pl.when(t >= 2)
        def _():
            late_out(t - 2).wait()

        h, scale = normed(x_t[slot])
        da = dot_as(dg_t[slot], ract[0:d, :], NT) + dot_as(du_t[slot], ract[d : 2 * d, :], NT)
        dx_t[slot] = through_norm(h, scale, da.astype(BF16).astype(F32), dh_t[slot])
        late_out(t).start()

    def end_wide(k):
        wide_out[k // wides, :, pl.ds(pl.multiple_of(lax.rem(k, wides) * COLS, COLS), COLS)] = wide.end(lax.rem(k, SLOTS))

    def end_down(r, j):
        down_out[r, :, pl.ds(pl.multiple_of(j * COLS, COLS), COLS)] = down.end(j)

    def send_wide(k):
        wide.middle(lax.rem(k, SLOTS))

    def send_down(r, j):
        down.middle(j)

    def due_wide(r, i):
        k = wides * r + i
        for lag, on_wide, on_down in ((ON, send_wide, send_down), (DONE, end_wide, end_down)):
            @pl.when(i >= lag)
            def _():
                on_wide(k - lag)

            @pl.when((r >= 1) & (i >= lag - downs) & (i < lag))
            def _():
                on_down(r - 1, i + downs - lag)

            if lag > downs:
                @pl.when((r >= 1) & (i < lag - downs))
                def _():
                    on_wide(k + downs - lag)

    def due_down(r, j):
        for lag, on_wide, on_down in ((ON, send_wide, send_down), (DONE, end_wide, end_down)):
            if lag < downs:
                @pl.when(j >= lag)
                def _():
                    on_down(r, j - lag)

            @pl.when((j < lag) & (wides + j >= lag))
            def _():
                on_wide(wides * r + wides + j - lag)

            if lag > wides:
                @pl.when((r >= 1) & (wides + j < lag))
                def _():
                    on_down(r - 1, downs + wides + j - lag)

    def wide_step(r, i, slot, tail):
        term[0:d, :] = dot_as(ra[...], blk[slot], TN)
        k = lax.rem(wides * r + i, SLOTS)
        wide.put(k, term)
        due_wide(r, i)
        wide.begin(k)
        tail()

    load_a1().start()
    load_wide(0, 0, 0)
    load_wd().start()
    barrier = pltpu.get_barrier_semaphore()
    for other in (wide.left, wide.right):
        pl.semaphore_signal(barrier, inc=1, device_id=other, device_id_type=pl.DeviceIdType.MESH)
    pl.semaphore_wait(barrier, 2)
    load_a1().wait()
    for c in tile_in(0):
        c.start()
    load_act1().start()
    load_wd().wait()

    def round_(r, _):
        def wide_block(i, _):
            q = (wides + downs) * r + i
            slot = lax.rem(q, 2)
            column(dg1, 0, slot).wait()

            @pl.when(i + 1 < wides)
            def _():
                load_wide(r, i + 1, 1 - slot)

            @pl.when(i + 1 == wides)
            def _():
                load_down(r, 0, 1 - slot)

            def tail():
                at = (i * first_tiles) // wides

                @pl.when(((i + 1) * first_tiles) // wides > at)
                def _():
                    tile(r * (tiles // 2) + at)

            wide_step(r, i, slot, tail)
            return 0

        lax.fori_loop(0, wides, wide_block, 0)

        @pl.when(r == 1)
        def _():
            load_a0().start()

        load_act1().wait()

        def down_block(j, _):
            q = (wides + downs) * r + wides + j
            slot = lax.rem(q, 2)
            column(dy, 0, slot).wait()

            @pl.when(j + 1 < downs)
            def _():
                load_down(r, j + 1, 1 - slot)

            @pl.when((j + 1 == downs) & (r == 0))
            def _():
                load_wide(r + 1, 0, 1 - slot)

            @pl.when((j + 1 == downs) & (r == 1))
            def _():
                for t in (tiles - 2, tiles - 1):
                    for c in tile_out(t):
                        c.wait()
                column(dg0, 0, 1 - slot).start()

            for s in cuts(ff, ff // 2):
                term[s, :] = dot_as(ract[:, s], blk[slot], TN)
            down.put(j, term)
            due_down(r, j)
            down.begin(j)

            @pl.when(j + 1 < downs)
            def _():
                tile(r * (tiles // 2) + first_tiles + j)

            return 0

        lax.fori_loop(0, downs, down_block, 0)

        @pl.when(r == 0)
        def _():
            load_act0().start()

        return 0

    lax.fori_loop(0, 2, round_, 0)

    last_q = 2 * (wides + downs)
    load_wg().start()
    load_wu().start()
    for c in late_in(0):
        c.start()
    load_a0().wait()
    blocks = 2 * wides
    late_early = tiles // 2

    def last_block(i, _):
        slot = lax.rem(last_q + i, 2)
        column(dg0, 0, slot).wait()

        @pl.when(i + 1 < blocks)
        def _():
            load_last(i + 1, 1 - slot)

        def tail():
            at = (i * late_early) // blocks

            @pl.when(((i + 1) * late_early) // blocks > at)
            def _():
                @pl.when(at == 0)
                def _():
                    load_wg().wait()
                    load_wu().wait()

                late(at)

        wide_step(2, i, slot, tail)
        return 0

    lax.fori_loop(0, blocks, last_block, 0)

    def rest(v, _):
        k = 2 * wides + blocks + v

        def one(t, _):
            late(late_early + t)
            return 0

        lax.fori_loop((v * late_early) // DONE, ((v + 1) * late_early) // DONE, one, 0)

        @pl.when(v < ON)
        def _():
            send_wide(k - ON)

        end_wide(k - DONE)
        return 0

    lax.fori_loop(0, DONE, rest, 0)
    for t in (tiles - 2, tiles - 1):
        late_out(t).wait()


def backward(n, dy, dh1, x, a0, a1, acts, act1, dg1, du1, g0, u0, wg0, wu0, wd0):
    rows, d = dy.shape
    ff = act1.shape[1]
    wide, down = d // n, ff // n
    assert n == 4 and rows // SMALL == 16 and d == 3 * COLS and ff == 7 * COLS
    anywhere = pl.BlockSpec(memory_space=pl.ANY)
    inside = pl.BlockSpec(memory_space=pltpu.VMEM)

    def slots(count, chunk):
        return [
            pltpu.VMEM((count, 3, chunk, COLS), F32),
            pltpu.VMEM((count, chunk, COLS), BF16),
            pltpu.VMEM((count, 2, chunk // 2, COLS), BF16),
            pltpu.VMEM((count, 2, chunk, COLS), BF16),
            pltpu.VMEM((count, 2, chunk, COLS), BF16),
        ]

    dma = pltpu.SemaphoreType.DMA
    return pl.pallas_call(
        functools.partial(backward_kernel, n, (rows, d, ff)),
        out_shape=[
            jax.ShapeDtypeStruct((4, wide, ff), BF16),
            jax.ShapeDtypeStruct((2, down, d), BF16),
            jax.ShapeDtypeStruct((rows, d), BF16),
            jax.ShapeDtypeStruct((rows, ff), BF16),
            jax.ShapeDtypeStruct((rows, ff), BF16),
        ],
        in_specs=[anywhere] * 14,
        out_specs=[inside, inside, anywhere, anywhere, anywhere],
        scratch_shapes=[
            pltpu.VMEM((rows, d), BF16),
            pltpu.VMEM((rows, ff), BF16),
            pltpu.VMEM((2, rows, COLS), BF16),
            pltpu.VMEM((ff, COLS), F32),
            pltpu.VMEM((ff, d), BF16),
            pltpu.VMEM((SMALL, ff), F32),
            pltpu.VMEM((SMALL, ff), F32),
            pltpu.VMEM((2, SMALL, d), BF16),
            pltpu.VMEM((2, SMALL, ff), BF16),
            pltpu.VMEM((2, SMALL, ff), BF16),
            pltpu.VMEM((2, SMALL, d), BF16),
            pltpu.VMEM((2, SMALL, d), BF16),
            *slots(SLOTS, wide),
            *slots(3, down),
            dma((SLOTS, 4)), dma((SLOTS, 4)), dma((3, 4)), dma((3, 4)),
            dma((2,)), dma((3,)), dma((4, 2)), dma((2, 2)),
        ],
        compiler_params=pltpu.CompilerParams(vmem_limit_bytes=67043328, collective_id=1, has_side_effects=True),
        cost_estimate=cost(9, rows, d, ff, 300 * 2**20),
        name="backward",
    )(dy, dh1, x, a0, a1, acts, act1, dg1, du1, g0, u0, wg0, wu0, wd0)


def solution(mesh):
    n = mesh.shape["dp"]

    def body(x, dy, sg, su, sd):
        x, dy = x[0], dy[0]
        h1, a0, acts, u0, g0, wg0, wu0, wd0, wg1, wu1 = forward(n, x, dy, sg, su, sd)
        dh1, a1, act1, dg1, du1 = last(h1, dy, acts, wg1, wu1)
        wide, down, dx, _, _ = backward(n, dy, dh1, x, a0, a1, acts, act1, dg1, du1, g0, u0, wg0, wu0, wd0)
        gate1, up1, gate0, up0 = wide
        down1, down0 = down
        return dx[None], jnp.stack([gate0, gate1]), jnp.stack([up0, up1]), jnp.stack([down0, down1])

    tokens = P(("rep", "dp"), None, None)
    return jax.shard_map(
        body,
        mesh=mesh,
        in_specs=(tokens, tokens) + (P(None, "dp", None),) * 3,
        out_specs=(tokens,) + (P("rep", "dp", None),) * 3,
        check_vma=False,
    )
```

```python
import functools

import jax
import jax.numpy as jnp
from jax import lax
from jax.experimental import pallas as pl
from jax.experimental.pallas import tpu as pltpu
from jax.sharding import PartitionSpec as P

F32, BF16 = jnp.float32, jnp.bfloat16
NT = (((1,), (1,)), ((), ()))
TN = (((0,), (0,)), ((), ()))
VMEM_LIMIT = 60 * 2**20
TILE = 512
COLS = 256
SMALL = 256
SLOTS = 9
ON, DONE = 4, 8
LAYERS = (1, 0, 0, 0, 1, 1)
EVENTS = {
    0: (("greet",), ("own", 0), ("neighbours", 0), ("own", 1), ("opposite", 0), ("own", 2), ("relay", 0), ("neighbours", 1), ("own", 3), ("complete", 0),),
    4: (("opposite", 1), ("neighbours", 2), ("own", 4),),
    6: (("relay", 1),),
    7: (("opposite", 2), ("neighbours", 3), ("own", 5),),
    8: (("complete", 1),),
    10: (("relay", 2),),
    11: (("opposite", 3),),
    13: (("neighbours", 4),),
    14: (("relay", 3),),
    15: (("opposite", 4), ("neighbours", 5),),
    16: (("complete", 2), ("complete", 3),),
    17: (("relay", 4), ("opposite", 5),),
    18: (("complete", 4),),
    19: (("relay", 5),),
    20: (("complete", 5),),
}


def dot(a, b):
    return jnp.dot(a, b, preferred_element_type=F32)


def dot_as(a, b, dims):
    return lax.dot_general(a, b, dims, preferred_element_type=F32)


def normed(h):
    wide = h.astype(F32)
    scale = lax.rsqrt(jnp.mean(wide * wide, -1, keepdims=True) + 1e-6)
    return wide, scale


def cuts(n, size):
    return [slice(at, min(at + size, n)) for at in range(0, n, size)]


def whole(shape):
    return pl.BlockSpec(shape, lambda *_: (0,) * len(shape), pipeline_mode=pl.Buffered(1))


def rows_of(width, tile=TILE):
    return pl.BlockSpec((tile, width), lambda i: (i, 0))


def params(**more):
    return pltpu.CompilerParams(dimension_semantics=("arbitrary",), vmem_limit_bytes=VMEM_LIMIT, **more)


def cost(matmuls, rows, d, ff, moved):
    return pl.CostEstimate(flops=2 * matmuls * rows * d * ff, bytes_accessed=moved, transcendentals=0)


class Gather:
    def __init__(self, n, shards, fulls, send, recv, local):
        self.n, self.shards, self.fulls, self.send, self.recv, self.local = n, shards, fulls, send, recv, local
        self.me = lax.axis_index("dp")
        rep = lax.axis_index("rep")
        core, chip = lax.rem(rep, 2), lax.rem(rep // 2, 2)
        self.outer = core == chip
        self.middle = core != chip
        self.bring, self.given, self.far = chip + core, chip + 1 - core, 2 - 2 * chip
        self.partner = {"rep": rep + 1 - 2 * core}
        self.twin = {"rep": rep + 2 - 4 * chip}
        self.right = {"dp": lax.rem(self.me + 1, n)}
        self.left = {"dp": lax.rem(self.me + n - 1, n)}

    def shard(self, m):
        return self.shards[m % 3].at[LAYERS[m]]

    def third(self, m, ref, row, which, part):
        block, width = self.shards[m % 3].shape[1:]
        if block % 6 == 0:
            rows = block // 3
            start, count = (0, rows) if part is None else (part * (rows // 2), rows // 2)
            return ref.at[pl.ds(pl.multiple_of(row + which * rows + start, 16), count)]
        columns = pl.ds(pl.multiple_of(which * (width // 3), 128), width // 3)
        start, count = (0, block) if part is None else (part * (block // 2), block // 2)
        return ref.at[pl.ds(pl.multiple_of(row + start, 16), count), columns]

    def piece(self, m, which, away, part=None):
        block = self.shards[m % 3].shape[1]
        return self.third(m, self.fulls[m], lax.rem(self.me + away + self.n, self.n) * block, which, part)

    def copy(self, m, k, src, dst, to):
        return pltpu.make_async_remote_copy(
            src_ref=src, dst_ref=dst, send_sem=self.send.at[m, k], recv_sem=self.recv.at[m, k],
            device_id=to, device_id_type=pl.DeviceIdType.MESH,
        )

    ARRIVALS = ((-1, None), (1, None), (2, 0), (2, 1))

    def ring(self, m, k):
        to = (self.right, self.left)[k % 2]
        if k < 2:
            return self.copy(m, k, self.third(m, self.shard(m), 0, self.bring, None), self.piece(m, self.bring, 0), to)
        ref = self.piece(m, self.bring, *((-1, 0), (1, 1))[k - 2])
        return self.copy(m, k, ref, ref, to)

    def hand(self, m, e, which, k, to):
        ref = self.piece(m, which, *self.ARRIVALS[e])
        return self.copy(m, k + e, ref, ref, to)

    def mine(self, m):
        block = self.shards[m % 3].shape[1]
        return pltpu.make_async_copy(self.shard(m), self.fulls[m].at[pl.ds(self.me * block, block)], self.local.at[m])

    def greet(self):
        barrier = pltpu.get_barrier_semaphore()
        for other in (self.left, self.right, self.partner, self.twin):
            pl.semaphore_signal(barrier, inc=1, device_id=other, device_id_type=pl.DeviceIdType.MESH)
        pl.semaphore_wait(barrier, 4)

    def own(self, m):
        for k in range(2):
            self.ring(m, k).start()
        self.mine(m).start()

    def arrived(self, m, e):
        self.hand(m, e, self.bring, 0, self.partner).wait_recv()
        if e < 2:
            self.ring(m, 2 + e).start()
        self.hand(m, e, self.bring, 4, self.partner).start()

        @pl.when(self.outer)
        def _():
            self.hand(m, e, self.bring, 8, self.twin).start()

    def neighbours(self, m):
        self.arrived(m, 0)
        self.arrived(m, 1)

    def opposite(self, m):
        self.arrived(m, 2)
        self.arrived(m, 3)

    def relay(self, m):
        @pl.when(self.middle)
        def _():
            for e in range(4):
                self.hand(m, e, self.far, 8, self.partner).wait_recv()
                self.hand(m, e, self.far, 8, self.partner).start()

    def complete(self, m):
        self.mine(m).wait()
        for e in range(4):
            self.hand(m, e, self.given, 4, self.partner).wait_recv()

        @pl.when(self.outer)
        def _():
            for e in range(4):
                self.hand(m, e, self.far, 8, self.partner).wait_recv()

    def sent(self, m):
        for k in range(4):
            self.ring(m, k).wait_send()
        for e in range(4):
            self.hand(m, e, self.bring, 4, self.partner).wait_send()
            self.hand(m, e, self.bring, 8, self.partner).wait_send()


def forward_kernel(n, x, dy, sd, sg, su, h1, a_out, acts, u_out, g_out, *rest):
    outs, fulls, (g_all, send, recv, local, out_sem, g_sem) = rest[:5], rest[5:11], rest[11:]
    gather = Gather(n, (sd, sg, su), fulls, send, recv, local)
    step = pl.program_id(0)
    tiles = pl.num_programs(0) // 3

    def keep(m):
        return pltpu.make_async_copy(fulls[m], outs[m - 1], out_sem.at[m - 1])

    def complete(m):
        gather.complete(m)
        if m:
            keep(m).start()

    for at, events in EVENTS.items():
        @pl.when(step == at)
        def _():
            for stage, *m in events:
                (complete if stage == "complete" else getattr(gather, stage))(*m)

    wd1, wg, wu, wd = fulls[:4]
    tile, ff = x.shape[0], wg.shape[1]

    def rows(t):
        return pl.ds(pl.multiple_of(t * tile, tile), tile)

    def keep_gate(t):
        return pltpu.make_async_copy(g_all.at[rows(t)], g_out.at[rows(t)], g_sem.at[t])

    @pl.when(step < tiles)
    def _():
        for s in cuts(ff, COLS):
            acts[0, :, s] = dot_as(dy[...], wd1[s, :], NT).astype(BF16)

    @pl.when((step >= tiles) & (step < 2 * tiles))
    def _():
        wide, scale = normed(x[...])
        a = (wide * scale).astype(BF16)
        a_out[...] = a
        for s in cuts(ff, COLS):
            g_all[rows(step - tiles), s] = dot(a, wg[:, s])
        keep_gate(step - tiles).start()

    @pl.when(step >= 2 * tiles)
    def _():
        h = x[...]
        wide, scale = normed(h)
        a = (wide * scale).astype(BF16)
        for s in cuts(ff, COLS):
            u = dot(a, wu[:, s])
            g = g_all[rows(step - 2 * tiles), s]
            u_out[:, s] = u
            acts[0, :, s] = (g * jax.nn.sigmoid(g) * u).astype(BF16)
        h1[...] = h + dot(acts[0], wd[...]).astype(BF16)

    @pl.when(step == pl.num_programs(0) - 1)
    def _():
        for m in range(6):
            gather.sent(m)
            if m:
                keep(m).wait()
        for t in range(8):
            keep_gate(t).wait()


def forward(n, x, dy, sg, su, sd):
    rows, d = x.shape
    ff = sg.shape[2]
    shapes = [(ff, d), (d, ff), (d, ff)] * 2
    tiles = rows // TILE
    assert tiles == 8 and n == 4
    outs = [((rows, d), BF16), ((rows, d), BF16), ((2, rows, ff), BF16), ((rows, ff), F32), ((rows, ff), F32)] + [(s, BF16) for s in shapes[1:]]
    anywhere = pl.BlockSpec(memory_space=pl.ANY)
    late = lambda width: pl.BlockSpec((TILE, width), lambda i: (jnp.maximum(i - 2 * tiles, 0), 0))
    dma = pltpu.SemaphoreType.DMA

    def acts_at(i):
        return jnp.where(i < 2 * tiles, 0, 1), jnp.where(i < 2 * tiles, jnp.minimum(i, tiles - 1), i - 2 * tiles), 0

    return pl.pallas_call(
        functools.partial(forward_kernel, n),
        grid=(3 * tiles,),
        out_shape=[jax.ShapeDtypeStruct(*o) for o in outs],
        in_specs=[
            pl.BlockSpec((TILE, d), lambda i: (lax.rem(i, tiles), 0)),
            pl.BlockSpec((TILE, d), lambda i: (jnp.minimum(i, tiles - 1), 0)),
        ]
        + [anywhere] * 3,
        out_specs=[
            late(d),
            pl.BlockSpec((TILE, d), lambda i: (jnp.clip(i - tiles, 0, tiles - 1), 0)),
            pl.BlockSpec((1, TILE, ff), acts_at),
            late(ff),
        ]
        + [anywhere] * 6,
        scratch_shapes=[pltpu.VMEM(s, BF16) for s in shapes]
        + [pltpu.VMEM((rows, ff), F32), dma((6, 12)), dma((6, 12)), dma((6,)), dma((5,)), dma((tiles,))],
        compiler_params=pltpu.CompilerParams(
            dimension_semantics=("arbitrary",), vmem_limit_bytes=67043328, collective_id=0, has_side_effects=True
        ),
        cost_estimate=cost(4, rows, d, ff, 130 * 2**20),
        name="forward",
    )(x, dy, sd, sg, su)


def through_norm(wide, scale, da, dh):
    m = jnp.mean(da * wide, -1, keepdims=True)
    return dh + (scale * da - wide * (scale * scale * scale * m)).astype(BF16)


def gate_grads(g, u, dact):
    sig = jax.nn.sigmoid(g)
    silu = g * sig
    return silu, (dact * u * (sig + silu * (1 - sig))).astype(BF16), (dact * silu).astype(BF16)


def last_kernel(h_ref, dy_ref, dacts, wg, wu, dh, a_out, act, dg, du):
    wide, scale = normed(h_ref[...])
    a = (wide * scale).astype(BF16)
    a_out[...] = a
    for s in cuts(wg.shape[1], COLS):
        g = dot(a, wg[:, s])
        u = dot(a, wu[:, s])
        silu, dg[:, s], du[:, s] = gate_grads(g, u, dacts[0, :, s].astype(F32))
        act[:, s] = (silu * u).astype(BF16)
    da = dot_as(dg[...], wg[...], NT) + dot_as(du[...], wu[...], NT)
    dh[...] = through_norm(wide, scale, da.astype(BF16).astype(F32), dy_ref[...])


def last(h, dy, acts, wg, wu):
    rows, d = h.shape
    ff = wg.shape[1]
    return pl.pallas_call(
        last_kernel,
        grid=(rows // TILE,),
        out_shape=[jax.ShapeDtypeStruct((rows, d), BF16)] * 2 + [jax.ShapeDtypeStruct((rows, ff), BF16)] * 3,
        in_specs=[rows_of(d), rows_of(d), pl.BlockSpec((1, TILE, ff), lambda i: (0, i, 0))] + [whole(w.shape) for w in (wg, wu)],
        out_specs=[rows_of(d)] * 2 + [rows_of(ff)] * 3,
        compiler_params=params(),
        cost_estimate=cost(4, rows, d, ff, 90 * 2**20),
        name="last",
    )(h, dy, acts, wg, wu)


class Scatter:
    def __init__(self, n, rows, keep, s1, r1, s2, r2, send, recv):
        self.rows, self.keep, self.s1, self.r1, self.s2, self.r2, self.send, self.recv = rows, keep, s1, r1, s2, r2, send, recv
        self.n = n
        self.me = lax.axis_index("dp")
        self.right = {"dp": lax.rem(self.me + 1, n)}
        self.left = {"dp": lax.rem(self.me + n - 1, n)}

    def copy(self, slot, k, src, dst):
        return pltpu.make_async_remote_copy(
            src_ref=src, dst_ref=dst, send_sem=self.send.at[slot, k], recv_sem=self.recv.at[slot, k],
            device_id=self.left if k % 2 else self.right, device_id_type=pl.DeviceIdType.MESH,
        )

    def opposites(self, slot, k):
        half = self.rows // 2
        return self.copy(slot, k, self.s1.at[slot, pl.ds(k * half, half)], self.r1.at[slot, k])

    def sums(self, slot, k):
        return self.copy(slot, 2 + k, self.s2.at[slot, k], self.r2.at[slot, k])

    def of(self, term, away):
        at = pl.multiple_of(lax.rem(self.me + away, self.n) * self.rows, 64)
        return term[pl.ds(at, self.rows), :]

    def put(self, slot, term):
        self.s1[slot] = self.of(term, 2).astype(BF16)
        self.keep[slot, 0] = self.of(term, 1)
        self.keep[slot, 1] = self.of(term, self.n - 1)
        self.keep[slot, 2] = self.of(term, 0)

    def begin(self, slot):
        for k in range(2):
            self.opposites(slot, k).start()

    def middle(self, slot):
        half = self.rows // 2
        for k in range(2):
            self.opposites(slot, k).wait_recv()
        for k in range(2):
            with_theirs, alone = pl.ds(k * half, half), pl.ds((1 - k) * half, half)
            self.s2[slot, k, with_theirs] = (self.keep[slot, k, with_theirs] + self.r1[slot, k].astype(F32)).astype(BF16)
            self.s2[slot, k, alone] = self.keep[slot, k, alone].astype(BF16)
        for k in range(2):
            self.sums(slot, k).start()

    def end(self, slot):
        for k in range(2):
            self.sums(slot, k).wait_recv()
        out = self.keep[slot, 2] + self.r2[slot, 0].astype(F32) + self.r2[slot, 1].astype(F32)
        for k in range(2):
            self.opposites(slot, k).wait_send()
            self.sums(slot, k).wait_send()
        return out.astype(BF16)


def backward_kernel(
    n, dims, dy, dh1, x, a0, a1, acts, act1, dg1, du1, g0, u0, wg0, wu0, wd0,
    wide_out, down_out, dx, dg0, du0,
    ra, ract, blk, term, wd, g_t, u_t, dh_t, dg_t, du_t, x_t, dx_t,
    wk, ws1, wr1, ws2, wr2, dk, ds1, dr1, ds2, dr2,
    wsend, wrecv, dsend, drecv, blk_sem, res_sem, in_sem, out_sem,
):
    rows, d, ff = dims
    tiles = rows // SMALL
    wides, downs = ff // COLS, d // COLS
    first_tiles = tiles // 2 - downs + 1
    wide = Scatter(n, d // n, wk, ws1, wr1, ws2, wr2, wsend, wrecv)
    down = Scatter(n, ff // n, dk, ds1, dr1, ds2, dr2, dsend, drecv)

    def resident(src, dst, k):
        return pltpu.make_async_copy(src, dst, res_sem.at[k])

    load_a1 = lambda: resident(a1, ra, 0)
    load_a0 = lambda: resident(a0, ra, 0)
    load_act1 = lambda: resident(act1, ract, 1)
    load_act0 = lambda: resident(acts.at[1], ract, 1)
    load_wd = lambda: resident(wd0, wd, 2)
    load_wg = lambda: resident(wg0, ract.at[pl.ds(0, d)], 1)
    load_wu = lambda: resident(wu0, ract.at[pl.ds(d, d)], 2)

    def column(src, j, slot):
        return pltpu.make_async_copy(src.at[:, pl.ds(pl.multiple_of(j * COLS, COLS), COLS)], blk.at[slot], blk_sem.at[slot])

    def load_wide(r, i, slot):
        for at, src in ((0, dg1), (1, du1)):
            @pl.when(r == at)
            def _():
                column(src, i, slot).start()

    def load_down(r, j, slot):
        for at, src in ((0, dy), (1, dh1)):
            @pl.when(r == at)
            def _():
                column(src, j, slot).start()

    def load_last(i, slot):
        @pl.when(i < wides)
        def _():
            column(dg0, i, slot).start()

        @pl.when(i >= wides)
        def _():
            column(du0, i - wides, slot).start()

    def tile_of(ref, t):
        return ref.at[pl.ds(pl.multiple_of(t * SMALL, SMALL), SMALL)]

    def tile_in(t):
        pairs = ((g0, g_t), (u0, u_t), (dh1, dh_t.at[0]))
        return [pltpu.make_async_copy(tile_of(src, t), dst, in_sem.at[k, 0]) for k, (src, dst) in enumerate(pairs)]

    def tile_out(t):
        slot = lax.rem(t, 2)
        return [pltpu.make_async_copy(src.at[slot], tile_of(dst, t), out_sem.at[k, slot]) for k, (src, dst) in enumerate(((dg_t, dg0), (du_t, du0)))]

    def tile(t):
        slot = lax.rem(t, 2)
        for c in tile_in(t):
            c.wait()

        @pl.when(t >= 2)
        def _():
            for c in tile_out(t - 2):
                c.wait()

        dh = dh_t[0]
        for s in cuts(ff, COLS):
            dact = dot_as(dh, wd[s, :], NT).astype(BF16).astype(F32)
            _, dg_t[slot, :, s], du_t[slot, :, s] = gate_grads(g_t[:, s], u_t[:, s], dact)

        @pl.when(t + 1 < tiles)
        def _():
            for c in tile_in(t + 1):
                c.start()

        for c in tile_out(t):
            c.start()

    def late_in(t):
        slot = lax.rem(t, 2)
        pairs = ((dg0, dg_t), (du0, du_t), (dh1, dh_t), (x, x_t))
        return [pltpu.make_async_copy(tile_of(src, t), dst.at[slot], in_sem.at[k, slot]) for k, (src, dst) in enumerate(pairs)]

    def late_out(t):
        slot = lax.rem(t, 2)
        return pltpu.make_async_copy(dx_t.at[slot], tile_of(dx, t), out_sem.at[0, slot])

    def late(t):
        slot = lax.rem(t, 2)
        for c in late_in(t):
            c.wait()

        @pl.when(t + 1 < tiles)
        def _():
            for c in late_in(t + 1):
                c.start()

        @pl.when(t >= 2)
        def _():
            late_out(t - 2).wait()

        h, scale = normed(x_t[slot])
        da = dot_as(dg_t[slot], ract[0:d, :], NT) + dot_as(du_t[slot], ract[d : 2 * d, :], NT)
        dx_t[slot] = through_norm(h, scale, da.astype(BF16).astype(F32), dh_t[slot])
        late_out(t).start()

    def end_wide(k):
        wide_out[k // wides, :, pl.ds(pl.multiple_of(lax.rem(k, wides) * COLS, COLS), COLS)] = wide.end(lax.rem(k, SLOTS))

    def end_down(r, j):
        down_out[r, :, pl.ds(pl.multiple_of(j * COLS, COLS), COLS)] = down.end(j)

    def send_wide(k):
        wide.middle(lax.rem(k, SLOTS))

    def send_down(r, j):
        down.middle(j)

    def due_wide(r, i):
        k = wides * r + i
        for lag, on_wide, on_down in ((ON, send_wide, send_down), (DONE, end_wide, end_down)):
            @pl.when(i >= lag)
            def _():
                on_wide(k - lag)

            @pl.when((r >= 1) & (i >= lag - downs) & (i < lag))
            def _():
                on_down(r - 1, i + downs - lag)

            if lag > downs:
                @pl.when((r >= 1) & (i < lag - downs))
                def _():
                    on_wide(k + downs - lag)

    def due_down(r, j):
        for lag, on_wide, on_down in ((ON, send_wide, send_down), (DONE, end_wide, end_down)):
            if lag < downs:
                @pl.when(j >= lag)
                def _():
                    on_down(r, j - lag)

            @pl.when((j < lag) & (wides + j >= lag))
            def _():
                on_wide(wides * r + wides + j - lag)

            if lag > wides:
                @pl.when((r >= 1) & (wides + j < lag))
                def _():
                    on_down(r - 1, downs + wides + j - lag)

    def wide_step(r, i, slot, tail):
        term[0:d, :] = dot_as(ra[...], blk[slot], TN)
        k = lax.rem(wides * r + i, SLOTS)
        wide.put(k, term)
        due_wide(r, i)
        wide.begin(k)
        tail()

    load_a1().start()
    load_wide(0, 0, 0)
    load_wd().start()
    barrier = pltpu.get_barrier_semaphore()
    for other in (wide.left, wide.right):
        pl.semaphore_signal(barrier, inc=1, device_id=other, device_id_type=pl.DeviceIdType.MESH)
    pl.semaphore_wait(barrier, 2)
    load_a1().wait()
    for c in tile_in(0):
        c.start()
    load_act1().start()
    load_wd().wait()

    def round_(r, _):
        def wide_block(i, _):
            q = (wides + downs) * r + i
            slot = lax.rem(q, 2)
            column(dg1, 0, slot).wait()

            @pl.when(i + 1 < wides)
            def _():
                load_wide(r, i + 1, 1 - slot)

            @pl.when(i + 1 == wides)
            def _():
                load_down(r, 0, 1 - slot)

            def tail():
                at = (i * first_tiles) // wides

                @pl.when(((i + 1) * first_tiles) // wides > at)
                def _():
                    tile(r * (tiles // 2) + at)

            wide_step(r, i, slot, tail)
            return 0

        lax.fori_loop(0, wides, wide_block, 0)

        @pl.when(r == 1)
        def _():
            load_a0().start()

        load_act1().wait()

        def down_block(j, _):
            q = (wides + downs) * r + wides + j
            slot = lax.rem(q, 2)
            column(dy, 0, slot).wait()

            @pl.when(j + 1 < downs)
            def _():
                load_down(r, j + 1, 1 - slot)

            @pl.when((j + 1 == downs) & (r == 0))
            def _():
                load_wide(r + 1, 0, 1 - slot)

            @pl.when((j + 1 == downs) & (r == 1))
            def _():
                for t in (tiles - 2, tiles - 1):
                    for c in tile_out(t):
                        c.wait()
                column(dg0, 0, 1 - slot).start()

            for s in cuts(ff, ff // 2):
                term[s, :] = dot_as(ract[:, s], blk[slot], TN)
            down.put(j, term)
            due_down(r, j)
            down.begin(j)

            @pl.when(j + 1 < downs)
            def _():
                tile(r * (tiles // 2) + first_tiles + j)

            return 0

        lax.fori_loop(0, downs, down_block, 0)

        @pl.when(r == 0)
        def _():
            load_act0().start()

        return 0

    lax.fori_loop(0, 2, round_, 0)

    last_q = 2 * (wides + downs)
    load_wg().start()
    load_wu().start()
    for c in late_in(0):
        c.start()
    load_a0().wait()
    blocks = 2 * wides
    late_early = tiles // 2

    def last_block(i, _):
        slot = lax.rem(last_q + i, 2)
        column(dg0, 0, slot).wait()

        @pl.when(i + 1 < blocks)
        def _():
            load_last(i + 1, 1 - slot)

        def tail():
            at = (i * late_early) // blocks

            @pl.when(((i + 1) * late_early) // blocks > at)
            def _():
                @pl.when(at == 0)
                def _():
                    load_wg().wait()
                    load_wu().wait()

                late(at)

        wide_step(2, i, slot, tail)
        return 0

    lax.fori_loop(0, blocks, last_block, 0)

    def rest(v, _):
        k = 2 * wides + blocks + v

        def one(t, _):
            late(late_early + t)
            return 0

        lax.fori_loop((v * late_early) // DONE, ((v + 1) * late_early) // DONE, one, 0)

        @pl.when(v < ON)
        def _():
            send_wide(k - ON)

        end_wide(k - DONE)
        return 0

    lax.fori_loop(0, DONE, rest, 0)
    for t in (tiles - 2, tiles - 1):
        late_out(t).wait()


def backward(n, dy, dh1, x, a0, a1, acts, act1, dg1, du1, g0, u0, wg0, wu0, wd0):
    rows, d = dy.shape
    ff = act1.shape[1]
    wide, down = d // n, ff // n
    assert n == 4 and rows // SMALL == 16 and d == 3 * COLS and ff == 7 * COLS
    anywhere = pl.BlockSpec(memory_space=pl.ANY)
    inside = pl.BlockSpec(memory_space=pltpu.VMEM)

    def slots(count, chunk):
        return [
            pltpu.VMEM((count, 3, chunk, COLS), F32),
            pltpu.VMEM((count, chunk, COLS), BF16),
            pltpu.VMEM((count, 2, chunk // 2, COLS), BF16),
            pltpu.VMEM((count, 2, chunk, COLS), BF16),
            pltpu.VMEM((count, 2, chunk, COLS), BF16),
        ]

    dma = pltpu.SemaphoreType.DMA
    return pl.pallas_call(
        functools.partial(backward_kernel, n, (rows, d, ff)),
        out_shape=[
            jax.ShapeDtypeStruct((4, wide, ff), BF16),
            jax.ShapeDtypeStruct((2, down, d), BF16),
            jax.ShapeDtypeStruct((rows, d), BF16),
            jax.ShapeDtypeStruct((rows, ff), BF16),
            jax.ShapeDtypeStruct((rows, ff), BF16),
        ],
        in_specs=[anywhere] * 14,
        out_specs=[inside, inside, anywhere, anywhere, anywhere],
        scratch_shapes=[
            pltpu.VMEM((rows, d), BF16),
            pltpu.VMEM((rows, ff), BF16),
            pltpu.VMEM((2, rows, COLS), BF16),
            pltpu.VMEM((ff, COLS), F32),
            pltpu.VMEM((ff, d), BF16),
            pltpu.VMEM((SMALL, ff), F32),
            pltpu.VMEM((SMALL, ff), F32),
            pltpu.VMEM((2, SMALL, d), BF16),
            pltpu.VMEM((2, SMALL, ff), BF16),
            pltpu.VMEM((2, SMALL, ff), BF16),
            pltpu.VMEM((2, SMALL, d), BF16),
            pltpu.VMEM((2, SMALL, d), BF16),
            *slots(SLOTS, wide),
            *slots(3, down),
            dma((SLOTS, 4)), dma((SLOTS, 4)), dma((3, 4)), dma((3, 4)),
            dma((2,)), dma((3,)), dma((4, 2)), dma((2, 2)),
        ],
        compiler_params=pltpu.CompilerParams(vmem_limit_bytes=67043328, collective_id=1, has_side_effects=True),
        cost_estimate=cost(9, rows, d, ff, 300 * 2**20),
        name="backward",
    )(dy, dh1, x, a0, a1, acts, act1, dg1, du1, g0, u0, wg0, wu0, wd0)


def solution(mesh):
    n = mesh.shape["dp"]

    def body(x, dy, sg, su, sd):
        x, dy = x[0], dy[0]
        h1, a0, acts, u0, g0, wg0, wu0, wd0, wg1, wu1 = forward(n, x, dy, sg, su, sd)
        dh1, a1, act1, dg1, du1 = last(h1, dy, acts, wg1, wu1)
        wide, down, dx, _, _ = backward(n, dy, dh1, x, a0, a1, acts, act1, dg1, du1, g0, u0, wg0, wu0, wd0)
        gate1, up1, gate0, up0 = wide
        down1, down0 = down
        return dx[None], jnp.stack([gate0, gate1]), jnp.stack([up0, up1]), jnp.stack([down0, down1])

    tokens = P(("rep", "dp"), None, None)
    return jax.shard_map(
        body,
        mesh=mesh,
        in_specs=(tokens, tokens) + (P(None, "dp", None),) * 3,
        out_specs=(tokens,) + (P("rep", "dp", None),) * 3,
        check_vma=False,
    )
```
